32 devices in a mesh: groups: 2 (over y), ep: 16 (over z, x, core).
Axes of the slice: x: 2, y: 2, z: 4, core: 2. Of those that a mesh axis runs over, the one named last changes fastest.
Arguments:
- tokens: bfloat16 [512, 2880], P(('groups', 'ep')), parts along dimension 0, may hold values from -6 to 6
- routes: int32 [512, 4], P(('groups', 'ep')), parts along dimension 0, may hold values from 0 to 7, all different within a row; in each aligned block of 16 rows (0 to 15, 16 to 31, ...) at most 16 rows name the same one
- gate_fixed: int32 [512, 4], P(('groups', 'ep')), parts along dimension 0, may hold values from 1 to 65535
- gate_weight: bfloat16 [16, 2880, 720], P('ep'), may hold values from -0.109375 to 0.109375
- up_weight: bfloat16 [16, 2880, 720], P('ep'), may hold values from -0.109375 to 0.109375
- down_weight: bfloat16 [16, 720, 2880], P('ep'), may hold values from -0.15625 to 0.15625
Outputs:
- mixed: bfloat16 [512, 2880], P(('groups', 'ep')), parts along dimension 0
The draws below stay inside these ranges and needn't reach their ends.
There are 2 independent parts, one for each index of `groups`. The reference program is written for one: setup_inputs(seed, part) draws one part's arguments, and reference() takes and returns one part's arrays. A program takes and returns all parts, laid end to end along the dimension named above; an argument that names none is the same for every part. Nothing has to cross between parts.
Inputs may be any that keep to these rules, and one draw needn't show every extreme that they name: `routes`: each row names 4 different experts; the 16 rows of one device name any one expert at most 16 times.
All inputs are finite; a program needn't handle non-finite values.
Results may differ from the reference program's by a relative error of at most 0.0065.
Values may be sent and summed in bfloat16 or wider, within the bound.
A program may use at most 64 MiB of HBM per device.

```python
import math
import jax
import jax.numpy as jnp
import numpy as np
from jax import lax

D = 2880
FF = 1440
TOP = 4
TOK_DEV = 16
HALF = 720
EXPERTS = 8
TOKENS = 256
CAP = 16
N_EP = 16


def set_ends(values, stream_key, least, high):
    longest = values.shape.index(max(values.shape))
    spots = []
    for shift in (0, 1):
        where = [jax.random.randint(jax.random.fold_in(stream_key, axis), (), 0, length) for axis, length in enumerate(values.shape)]
        where[longest] = (where[longest] + shift) % values.shape[longest]
        spots.append(tuple(where))
    return values.at[spots[0]].set(least).at[spots[1]].set(high)


def block_levels(rng, extent, split, least, top_value):
    level, own = 1.0, jax.random.fold_in(rng, 6)
    for dim, parts in split:
        steps = jnp.exp(jax.random.uniform(jax.random.fold_in(own, dim), (parts,), jnp.float32, least / len(split), top_value / len(split)))
        level = level * jnp.repeat(steps, extent[dim] // parts).reshape([-1 if axis == dim else 1 for axis in range(len(extent))])
    return level


def shared_out(stream_key, own, number, rows, amount, top, reach, lean):
    sequence = jax.random.permutation(stream_key, amount)
    heavy_load, ordinary = shares(amount, rows * top, reach, lean, True), shares(amount, rows * top, reach, lean, False)
    places = jnp.arange(amount)

    def named(lengths, turn):
        used = int((lengths > 0).sum())
        fixed = max(1, used // 4)
        moved = fixed + (places - fixed + turn * (used - fixed)) % max(1, amount - fixed)
        return jnp.zeros((amount,), jnp.int32).at[sequence[jnp.where(places < fixed, places, moved)]].set(jnp.asarray(lengths, jnp.int32))

    lengths = jnp.where(number % 4 == 0, named(heavy_load, number // 4), named(ordinary, number - number // 4 - 1))
    mixed = jax.random.permutation(jax.random.fold_in(own, 3), amount)
    giver, receiver = mixed[0:amount // 2 * 2:2], mixed[1:amount // 2 * 2:2]
    margin = jnp.minimum(lengths[giver] - 1, reach - lengths[receiver]) // 2
    margin = jnp.where((giver == sequence[0]) | (receiver == sequence[0]) | (lengths[receiver] == 0), 0, jnp.maximum(margin, 0))
    moved = jax.random.randint(jax.random.fold_in(own, 4), (amount // 2,), 0, 1 << 20) % (margin + 1)
    lengths = lengths.at[giver].add(-moved).at[receiver].add(moved)
    members = jnp.searchsorted(jnp.cumsum(lengths), jnp.arange(rows * top), side="right").astype(jnp.int32)
    grid = members.reshape(top, rows).T
    grid = grid[jax.random.permutation(jax.random.fold_in(own, 1), rows)]
    turn = jax.random.randint(jax.random.fold_in(own, 2), (rows, 1), 0, top)
    return jnp.take_along_axis(grid, (jnp.arange(top)[None, :] + turn) % top, axis=1)


def shares(count, total, limit, lean, full):
    weights = [(1 << 20) // math.isqrt(standing ** lean) + 1 for standing in range(1, count + 1)]
    largest = limit if full else min(limit, max(-(-total // count), total * weights[0] // sum(weights)))
    least = 1 if total - largest >= count - 1 else 0
    given, surplus = [largest] + [least] * (count - 1), total - largest - least * (count - 1)
    while surplus > 0:
        free = [i for i in range(1, count) if given[i] < largest] or [i for i in range(1, count) if given[i] < limit]
        pool, budget = sum([weights[i] for i in free]), surplus
        for i in free:
            more = min(limit - given[i], max(1, budget * weights[i] // pool), surplus)
            given[i] = given[i] + more
            surplus = surplus - more
    return np.array(given)


def noise(own_key, dims, spread, limit, shards=(), kind=jnp.bfloat16):
    drawn = jax.random.normal(own_key, dims, jnp.float32) * spread
    if len(shards) > 0:
        drawn = block_levels(own_key, dims, shards, -0.22, 0.18) * drawn
    return jnp.clip(drawn, min=-limit, max=limit).astype(kind)


def setup_inputs(seed: int = 0, part: int = 0) -> dict:
    streams_of = jax.random.split(jax.random.key(seed), 7)
    part_keys = jax.random.split(jax.random.fold_in(streams_of[6], part), 7)
    tokens = noise(part_keys[0], (TOKENS, D), 1.0, 6.0, ((0, 16),))
    routes_keys = jax.random.split(jax.random.fold_in(part_keys[1], 1), TOKENS // TOK_DEV)
    routes_turns = jax.random.permutation(jax.random.fold_in(part_keys[1], 3), TOKENS // TOK_DEV)
    routes = jax.vmap(lambda own, number: shared_out(jax.random.fold_in(part_keys[1], 2), own, number, TOK_DEV, EXPERTS, TOP, CAP, 2))(routes_keys, routes_turns).reshape((TOKENS, TOP))
    gate_fixed = set_ends(jax.random.randint(part_keys[2], (TOKENS, TOP), 1, 65536), jax.random.fold_in(part_keys[2], 1), 1, 65535).astype(jnp.int32)
    gate_weight = noise(streams_of[3], (N_EP, D, HALF), D ** -0.5, 0.109375, ((0, 16),))
    up_weight = noise(streams_of[4], (N_EP, D, HALF), D ** -0.5, 0.109375, ((0, 16),))
    down_weight = noise(streams_of[5], (N_EP, HALF, D), FF ** -0.5, 0.15625, ((0, 16),))
    return dict(tokens=tokens, routes=routes, gate_fixed=gate_fixed, gate_weight=gate_weight, up_weight=up_weight, down_weight=down_weight)


def reference(tokens, routes, gate_fixed, gate_weight, up_weight, down_weight):
    experts = N_EP // 2
    onehot = (routes[:, :, None] == jnp.arange(experts, dtype=jnp.int32)).astype(jnp.int32)
    grouped = onehot.reshape(N_EP, TOK_DEV * TOP, experts)
    before = jnp.cumsum(grouped, axis=1) - grouped
    position = jnp.sum(before * grouped, axis=-1).reshape(TOKENS, TOP).astype(jnp.int32)
    source = (jnp.arange(TOKENS, dtype=jnp.int32) // TOK_DEV)[:, None]
    column = (source * CAP + position).astype(jnp.int32)
    token_ids = jnp.broadcast_to(jnp.arange(TOKENS, dtype=jnp.int32)[:, None], (TOKENS, TOP))
    slot_table = jnp.full((experts, N_EP * CAP), TOKENS, jnp.int32).at[routes, column].set(token_ids)
    padded = jnp.concatenate([tokens, jnp.zeros((1, D), tokens.dtype)], axis=0)

    def half_part(expert_rows, index):
        w_gate = lax.dynamic_index_in_dim(gate_weight, index, 0, keepdims=False)
        w_up = lax.dynamic_index_in_dim(up_weight, index, 0, keepdims=False)
        w_down = lax.dynamic_index_in_dim(down_weight, index, 0, keepdims=False)
        gate_part = jnp.dot(expert_rows, w_gate, preferred_element_type=jnp.float32)
        up_part = jnp.dot(expert_rows, w_up, preferred_element_type=jnp.float32)
        hidden = (jax.nn.silu(gate_part) * up_part).astype(jnp.bfloat16)
        return jnp.dot(hidden, w_down, preferred_element_type=jnp.float32).astype(jnp.bfloat16)

    def run_expert(expert):
        expert_rows = padded[slot_table[expert]]
        first = (2 * expert).astype(jnp.int32)
        lower = half_part(expert_rows, first)
        upper = half_part(expert_rows, (first + 1).astype(jnp.int32))
        return (lower.astype(jnp.float32) + upper.astype(jnp.float32)).astype(jnp.bfloat16)

    outputs = lax.map(run_expert, jnp.arange(experts, dtype=jnp.int32))
    picked = outputs[routes, column]
    weights = gate_fixed.astype(jnp.float32) / 65536.0
    mixed = jnp.sum(weights[:, :, None] * picked.astype(jnp.float32), axis=1)
    return mixed.astype(jnp.bfloat16)
```

```python
import jax
import jax.numpy as jnp
from jax import lax
from jax.experimental import pallas as pl
from jax.experimental.pallas import tpu as pltpu
from jax.sharding import PartitionSpec as P


def swapped(value, axis, bit):
    mask = 2**bit
    pairs = [(source, source ^ mask) for source in range(lax.axis_size(axis))]
    return lax.ppermute(value, axis, pairs)


def expert_half(expert_rows, w_gate, w_up, w_down):
    gate_part = jnp.dot(expert_rows, w_gate, preferred_element_type=jnp.float32)
    up_part = jnp.dot(expert_rows, w_up, preferred_element_type=jnp.float32)
    hidden = (jax.nn.silu(gate_part) * up_part).astype(jnp.bfloat16)
    return jnp.dot(hidden, w_down, preferred_element_type=jnp.float32).astype(jnp.bfloat16)


def local(tokens, routes, gate_fixed, gate_weight, up_weight, down_weight):
    devices_ep = lax.axis_size("ep")
    experts = devices_ep // 2
    tok_count = tokens.shape[0]
    top_count = routes.shape[1]
    width = tokens.shape[1]
    capacity = 2 * tok_count * top_count // experts
    onehot = (routes[:, :, None] == jnp.arange(experts, dtype=jnp.int32)).astype(jnp.int32)
    flat_hot = onehot.reshape(tok_count * top_count, experts)
    before = jnp.cumsum(flat_hot, axis=0) - flat_hot
    position = jnp.sum(before * flat_hot, axis=1).reshape(tok_count, top_count)
    slot_index = routes * capacity + position
    select = (slot_index[:, :, None] == jnp.arange(experts * capacity, dtype=jnp.int32)).astype(
        jnp.int32
    )
    select = jnp.sum(select, axis=1).astype(jnp.bfloat16)
    packed = jnp.einsum("ts,td->sd", select, tokens, preferred_element_type=jnp.float32).astype(
        jnp.bfloat16
    )
    packed = packed.reshape(experts, 1, capacity, width)
    outgoing = jnp.broadcast_to(packed, (experts, 2, capacity, width)).reshape(
        devices_ep, capacity, width
    )
    received = lax.all_to_all(outgoing, "ep", split_axis=0, concat_axis=0, tiled=True)
    result = expert_half(received.reshape(-1, width), gate_weight[0], up_weight[0], down_weight[0])
    partial_value = result.reshape(received.shape[0], received.shape[1], width)
    parity = lax.axis_index("ep") % 2
    halves = partial_value.reshape(devices_ep, capacity, 2, width // 2)
    kept_half = lax.dynamic_index_in_dim(halves, parity, 2, keepdims=False)
    given_half = lax.dynamic_index_in_dim(halves, 1 - parity, 2, keepdims=False)
    partner = swapped(given_half, "ep", 0)
    reduced = (kept_half.astype(jnp.float32) + partner.astype(jnp.float32)).astype(jnp.bfloat16)
    returned = lax.all_to_all(reduced, "ep", split_axis=0, concat_axis=0, tiled=True)
    ordered = returned.reshape(experts, 2, capacity, width // 2).transpose(0, 2, 1, 3)
    expert_out = ordered.reshape(experts * capacity, width)
    picked = jnp.take(expert_out, slot_index.reshape(-1), axis=0).reshape(
        tok_count, top_count, width
    )
    weights = gate_fixed.astype(jnp.float32) / 65536.0
    mixed = jnp.sum(weights[:, :, None] * picked.astype(jnp.float32), axis=1)
    return mixed.astype(jnp.bfloat16)


NT = (((1,), (1,)), ((), ()))
TN = (((0,), (0,)), ((), ()))


def column_cuts(width, step):
    return [(low, min(low + step, width)) for low in range(0, width, step)]


def quad_kernel(
    tokens, routes, gates, w_gate, w_up, w_down, out,
    own_tokens, own_routes, own_gates, gathered, vm_gate, vm_up, vm_down, gate_sum, up_sum, partial, from_core,
    to_quad, from_quad, kept, to_far, from_far,
    in_sem, w_sem, ag_send, ag_recv, core_send, core_recv, quad_send, quad_recv, far_send, far_recv,
):
    rows, width = own_tokens.shape
    top = own_routes.shape[0]
    padded = gathered.shape[1]
    hidden_count = vm_gate.shape[0]
    device = lax.axis_index("ep")
    expert = (device // 2).astype(jnp.float32)

    def other(mask):
        return device + mask * (1 - 2 * lax.rem(device // mask, 2))

    core_peer = other(1)
    far_peer = other(8)
    side_peer = other(2)
    pair_peer = other(4)
    diagonal = side_peer + pair_peer - device
    quad_peers = [None, side_peer, pair_peer, diagonal]

    def send(source, target, send_sem, recv_sem, device_id):
        return pltpu.make_async_remote_copy(
            src_ref=source, dst_ref=target, send_sem=send_sem, recv_sem=recv_sem,
            device_id={"ep": device_id}, device_id_type=pl.DeviceIdType.MESH,
        )

    peers = [core_peer, side_peer, pair_peer, diagonal, far_peer]
    barrier = pltpu.get_barrier_semaphore()
    for peer in peers:
        pl.semaphore_signal(
            barrier, inc=1, device_id={"ep": peer}, device_id_type=pl.DeviceIdType.MESH
        )

    inputs = [
        pltpu.make_async_copy(source, target, in_sem.at[i])
        for i, (source, target) in enumerate(
            ((tokens, own_tokens), (routes, own_routes), (gates, own_gates))
        )
    ]
    weights = [
        pltpu.make_async_copy(source.at[0], target, w_sem.at[i])
        for i, (source, target) in enumerate(((w_gate, vm_gate), (w_up, vm_up), (w_down, vm_down)))
    ]
    for copy in inputs:
        copy.start()

    block_rows = 4 * rows
    chunk_rows = 2 * block_rows
    edge = width // 128 * 128
    step = -(-(padded // 128) // PIECES) * 128
    cuts = column_cuts(padded, step)

    def slot(chunk, core, q):
        return pl.ds(chunk * chunk_rows + core * block_rows + q * rows, rows)

    for copy in inputs:
        copy.wait()
    for copy in weights:
        copy.start()
    lanes = lax.broadcasted_iota(jnp.int32, (rows, padded - edge), 1) + edge
    mine = slot(0, 0, 0)
    partial[:, edge:] = jnp.zeros((2 * chunk_rows, padded - edge), jnp.bfloat16)
    gathered[mine, :edge] = own_tokens[:, :edge]
    gathered[mine, edge:] = jnp.zeros((rows, padded - edge), jnp.bfloat16)
    gathered[mine, edge:width] = own_tokens[:, edge:]
    scale = jnp.transpose(own_gates[...].astype(jnp.float32)) / 65536.0
    high = scale.astype(jnp.bfloat16).astype(jnp.float32)
    low = scale - high
    ids = jnp.transpose(own_routes[...].astype(jnp.float32))
    tail = gathered[mine, edge:].astype(jnp.float32)
    for k in range(top):
        tail = jnp.where(lanes == width + k, ids[:, k : k + 1], tail)
        tail = jnp.where(lanes == width + top + k, high[:, k : k + 1], tail)
        tail = jnp.where(lanes == width + 2 * top + k, low[:, k : k + 1], tail)
    gathered[mine, edge:] = tail.astype(jnp.bfloat16)

    with jax.named_scope("barrier"):
        pl.semaphore_wait(barrier, len(peers))

    started = []

    def launch(copy):
        copy.start()
        started.append(copy)

    def moved(chunk, core, q, piece, origin, peer):
        low_col, high_col = cuts[piece]
        return send(
            gathered.at[origin, low_col:high_col], gathered.at[slot(chunk, core, q), low_col:high_col],
            ag_send.at[chunk, core, q, piece], ag_recv.at[chunk, core, q, piece], peer,
        )

    def arrived(chunk, core, q, piece):
        moved(chunk, core, q, piece, slot(chunk, core, q), core_peer).wait_recv()

    def to_core(chunk, q, piece):
        launch(moved(chunk, 1, q, piece, slot(chunk, 0, q), core_peer))

    pieces = range(len(cuts))
    for piece in pieces:
        launch(moved(1, 0, 0, piece, mine, far_peer))
    for piece in pieces:
        for q in (2, 1) if RELAY else (2, 1, 3):
            launch(moved(0, 0, q, piece, mine, quad_peers[q]))
        to_core(0, 0, piece)

    def take_near(piece):
        for q in (2, 1) if RELAY else (2, 1, 3):
            arrived(0, 0, q, piece)
            if RELAY and q == 2:
                launch(moved(0, 0, 3, piece, slot(0, 0, 2), side_peer))
            to_core(0, q, piece)

    def take_far(piece):
        arrived(1, 0, 0, piece)
        for q in (3, 2, 1):
            launch(moved(1, 0, q, piece, slot(1, 0, 0), quad_peers[q]))
        to_core(1, 0, piece)

    def chunk_slice(chunk):
        return pl.ds(chunk * chunk_rows, chunk_rows)

    def core_copy(chunk, piece):
        low_col, high_col = cuts[piece]
        start = chunk * chunk_rows
        return send(
            partial.at[pl.ds(start + block_rows, block_rows), low_col:high_col],
            from_core.at[pl.ds(chunk * block_rows, block_rows), low_col:high_col],
            core_send.at[chunk, piece], core_recv.at[chunk, piece], core_peer,
        )

    def add_products(piece):
        low_col, high_col = cuts[piece][0], min(cuts[piece][1], width)
        x = gathered[:, low_col:high_col]
        for weight, total in ((vm_gate, gate_sum), (vm_up, up_sum)):
            product = lax.dot_general(
                weight[:, low_col:high_col], x, NT, preferred_element_type=jnp.float32
            )
            total[...] = product if piece == 0 else total[...] + product

    def gate_factor():
        info = gathered[:, edge:].astype(jnp.float32)
        factor = jnp.zeros((2 * chunk_rows, 1), jnp.float32)
        for k in range(top):
            col = width - edge + k
            value = info[:, col + top : col + top + 1] + info[:, col + 2 * top : col + 2 * top + 1]
            factor += jnp.where(info[:, col : col + 1] == expert, value, 0.0)
        return factor

    def run_down(hidden, factor, piece):
        start, stop = cuts[piece]
        for low_col in range(start, min(stop, width), 512):
            high_col = min(low_col + 512, stop, width)
            y = lax.dot_general(
                hidden, vm_down[:, low_col:high_col], TN, preferred_element_type=jnp.float32
            )
            partial[:, low_col:high_col] = (y * factor).astype(jnp.bfloat16)
        for chunk in (1, 0):
            launch(core_copy(chunk, piece))

    def quad_slot(chunk, q):
        return pl.ds((chunk * 3 + q - 1) * rows, rows)

    def quad_copy(chunk, q, piece):
        low_col, high_col = cuts[piece]
        where = quad_slot(chunk, q)
        return send(
            to_quad.at[where, low_col:high_col], from_quad.at[where, low_col:high_col],
            quad_send.at[chunk, q, piece], quad_recv.at[chunk, q, piece], quad_peers[q],
        )

    def give_quad(chunk, piece):
        low_col, high_col = cuts[piece]
        core_copy(chunk, piece).wait_recv()
        for q in (3, 2, 1, 0):
            total = partial[slot(chunk, 0, q), low_col:high_col].astype(jnp.float32)
            total += from_core[pl.ds(chunk * block_rows + q * rows, rows), low_col:high_col].astype(jnp.float32)
            if q == 0:
                kept[pl.ds(chunk * rows, rows), low_col:high_col] = total
            else:
                to_quad[quad_slot(chunk, q), low_col:high_col] = total.astype(jnp.bfloat16)
                launch(quad_copy(chunk, q, piece))

    def quad_total(chunk, piece):
        low_col, high_col = cuts[piece]
        total = kept[pl.ds(chunk * rows, rows), low_col:high_col]
        for q in (1, 2, 3):
            quad_copy(chunk, q, piece).wait_recv()
            total += from_quad[quad_slot(chunk, q), low_col:high_col].astype(jnp.float32)
        return total

    def far_copy(piece):
        low_col, high_col = cuts[piece]
        return send(
            to_far.at[:, low_col:high_col], from_far.at[:, low_col:high_col],
            far_send.at[piece], far_recv.at[piece], far_peer,
        )

    def take_quad(piece):
        if RELAY:
            arrived(0, 0, 3, piece)
            to_core(0, 3, piece)
        for q in (1, 2, 3):
            arrived(1, 0, q, piece)
            to_core(1, q, piece)

    def take_core(piece):
        for chunk in (0, 1):
            for q in range(4):
                arrived(chunk, 1, q, piece)

    last = len(cuts) - 1
    for piece in pieces:
        with jax.named_scope(f"near{piece}"):
            take_near(piece)
        with jax.named_scope(f"far{piece}"):
            take_far(piece)
        if piece > 0:
            with jax.named_scope(f"quad{piece - 1}"):
                take_quad(piece - 1)
    weights[0].wait()
    weights[1].wait()
    for piece in pieces:
        with jax.named_scope(f"core{piece}"):
            take_core(piece)
        with jax.named_scope(f"dot{piece}"):
            add_products(piece)
        if piece == last - 1:
            with jax.named_scope(f"quad{last}"):
                take_quad(last)
    with jax.named_scope("silu"):
        hidden = (jax.nn.silu(gate_sum[...]) * up_sum[...]).astype(jnp.bfloat16)
        factor = gate_factor()
    weights[2].wait()
    for piece in pieces:
        with jax.named_scope(f"down{piece}"):
            run_down(hidden, factor, piece)
    with jax.named_scope("give1"):
        for piece in pieces:
            give_quad(1, piece)
    with jax.named_scope("give0"):
        for piece in pieces:
            give_quad(0, piece)
    with jax.named_scope("far_out"):
        for piece in pieces:
            low_col, high_col = cuts[piece]
            to_far[:, low_col:high_col] = quad_total(1, piece).astype(jnp.bfloat16)
            launch(far_copy(piece))
    with jax.named_scope("final"):
        for piece in pieces:
            low_col, high_col = cuts[piece]
            total = quad_total(0, piece)
            far_copy(piece).wait_recv()
            total += from_far[:, low_col:high_col].astype(jnp.float32)
            high_col = min(high_col, width)
            out[:, low_col:high_col] = total[:, : high_col - low_col].astype(out.dtype)
    for copy in started:
        copy.wait_send()


PIECES = 3
RELAY = True


def quad_local(tokens, routes, gate_fixed, gate_weight, up_weight, down_weight):
    rows, width = tokens.shape
    top = routes.shape[1]
    gate_weight = jnp.swapaxes(gate_weight, 1, 2)
    up_weight = jnp.swapaxes(up_weight, 1, 2)
    padded = -(-(width + 3 * top) // 128) * 128
    dma = pltpu.SemaphoreType.DMA
    anywhere = pl.BlockSpec(memory_space=pl.ANY)
    routes, gate_fixed = routes.T, gate_fixed.T
    return pl.pallas_call(
        quad_kernel,
        out_shape=pltpu.VMEM((rows, width), jnp.bfloat16),
        in_specs=[anywhere] * 6,
        out_specs=pl.BlockSpec(memory_space=pltpu.VMEM),
        scratch_shapes=[
            pltpu.VMEM(tokens.shape, jnp.bfloat16),
            pltpu.VMEM(routes.shape, jnp.int32),
            pltpu.VMEM(gate_fixed.shape, jnp.int32),
            pltpu.VMEM((16 * rows, padded), jnp.bfloat16),
            pltpu.VMEM(gate_weight.shape[1:], jnp.bfloat16),
            pltpu.VMEM(up_weight.shape[1:], jnp.bfloat16),
            pltpu.VMEM(down_weight.shape[1:], jnp.bfloat16),
            pltpu.VMEM((gate_weight.shape[1], 16 * rows), jnp.float32),
            pltpu.VMEM((gate_weight.shape[1], 16 * rows), jnp.float32),
            pltpu.VMEM((16 * rows, padded), jnp.bfloat16),
            pltpu.VMEM((8 * rows, padded), jnp.bfloat16),
            pltpu.VMEM((6 * rows, padded), jnp.bfloat16),
            pltpu.VMEM((6 * rows, padded), jnp.bfloat16),
            pltpu.VMEM((2 * rows, padded), jnp.float32),
            pltpu.VMEM((rows, padded), jnp.bfloat16),
            pltpu.VMEM((rows, padded), jnp.bfloat16),
            dma((3,)), dma((3,)),
            dma((2, 2, 4, PIECES)), dma((2, 2, 4, PIECES)),
            dma((2, PIECES)), dma((2, PIECES)),
            dma((2, 4, PIECES)), dma((2, 4, PIECES)),
            dma((PIECES,)), dma((PIECES,)),
        ],
        compiler_params=pltpu.CompilerParams(
            collective_id=0, has_side_effects=True, vmem_limit_bytes=60 * 2**20
        ),
    )(tokens, routes, gate_fixed, gate_weight, up_weight, down_weight)


def solution(mesh):
    placed = (
        P(("groups", "ep"), None),
        P(("groups", "ep"), None),
        P(("groups", "ep"), None),
        P("ep", None, None),
        P("ep", None, None),
        P("ep", None, None),
    )
    chips = mesh.shape["ep"] // 2

    def body(*args):
        if chips == 2**3:
            return quad_local(*args)
        return local(*args)

    return jax.shard_map(
        body, mesh=mesh, in_specs=placed, out_specs=P(("groups", "ep"), None), check_vma=False
    )
```

```python
import jax
import jax.numpy as jnp
from jax import lax
from jax.experimental import pallas as pl
from jax.experimental.pallas import tpu as pltpu
from jax.sharding import PartitionSpec as P


def swapped(value, axis, bit):
    mask = 2**bit
    pairs = [(source, source ^ mask) for source in range(lax.axis_size(axis))]
    return lax.ppermute(value, axis, pairs)


def expert_half(expert_rows, w_gate, w_up, w_down):
    gate_part = jnp.dot(expert_rows, w_gate, preferred_element_type=jnp.float32)
    up_part = jnp.dot(expert_rows, w_up, preferred_element_type=jnp.float32)
    hidden = (jax.nn.silu(gate_part) * up_part).astype(jnp.bfloat16)
    return jnp.dot(hidden, w_down, preferred_element_type=jnp.float32).astype(jnp.bfloat16)


def local(tokens, routes, gate_fixed, gate_weight, up_weight, down_weight):
    devices_ep = lax.axis_size("ep")
    experts = devices_ep // 2
    tok_count = tokens.shape[0]
    top_count = routes.shape[1]
    width = tokens.shape[1]
    capacity = 2 * tok_count * top_count // experts
    onehot = (routes[:, :, None] == jnp.arange(experts, dtype=jnp.int32)).astype(jnp.int32)
    flat_hot = onehot.reshape(tok_count * top_count, experts)
    before = jnp.cumsum(flat_hot, axis=0) - flat_hot
    position = jnp.sum(before * flat_hot, axis=1).reshape(tok_count, top_count)
    slot_index = routes * capacity + position
    select = (slot_index[:, :, None] == jnp.arange(experts * capacity, dtype=jnp.int32)).astype(
        jnp.int32
    )
    select = jnp.sum(select, axis=1).astype(jnp.bfloat16)
    packed = jnp.einsum("ts,td->sd", select, tokens, preferred_element_type=jnp.float32).astype(
        jnp.bfloat16
    )
    packed = packed.reshape(experts, 1, capacity, width)
    outgoing = jnp.broadcast_to(packed, (experts, 2, capacity, width)).reshape(
        devices_ep, capacity, width
    )
    received = lax.all_to_all(outgoing, "ep", split_axis=0, concat_axis=0, tiled=True)
    result = expert_half(received.reshape(-1, width), gate_weight[0], up_weight[0], down_weight[0])
    partial_value = result.reshape(received.shape[0], received.shape[1], width)
    parity = lax.axis_index("ep") % 2
    halves = partial_value.reshape(devices_ep, capacity, 2, width // 2)
    kept_half = lax.dynamic_index_in_dim(halves, parity, 2, keepdims=False)
    given_half = lax.dynamic_index_in_dim(halves, 1 - parity, 2, keepdims=False)
    partner = swapped(given_half, "ep", 0)
    reduced = (kept_half.astype(jnp.float32) + partner.astype(jnp.float32)).astype(jnp.bfloat16)
    returned = lax.all_to_all(reduced, "ep", split_axis=0, concat_axis=0, tiled=True)
    ordered = returned.reshape(experts, 2, capacity, width // 2).transpose(0, 2, 1, 3)
    expert_out = ordered.reshape(experts * capacity, width)
    picked = jnp.take(expert_out, slot_index.reshape(-1), axis=0).reshape(
        tok_count, top_count, width
    )
    weights = gate_fixed.astype(jnp.float32) / 65536.0
    mixed = jnp.sum(weights[:, :, None] * picked.astype(jnp.float32), axis=1)
    return mixed.astype(jnp.bfloat16)


NT = (((1,), (1,)), ((), ()))
TN = (((0,), (0,)), ((), ()))


def column_cuts(low, high, step):
    return [(start, min(start + step, high)) for start in range(low, high, step)]


def portions(padded, shares):
    tiles = padded // 128
    ends = [tiles * sum(shares[:i]) // sum(shares) * 128 for i in range(len(shares) + 1)]
    return list(zip(ends[:-1], ends[1:]))


NT = (((1,), (1,)), ((), ()))
TN = (((0,), (0,)), ((), ()))
IN_SHARES = (8, 8, 7)
OUT_SHARES = (8, 8, 7)


def quad_kernel(
    tokens, routes, gates, w_gate, w_up, w_down, out,
    own_tokens, own_routes, own_gates, gathered, vm_gate, vm_up, vm_down, gate_sum, up_sum, partial,
    from_core, to_quad, from_quad, kept, to_far, from_far,
    in_sem, w_sem, sent, near_sem, far_sem, late_sem, core_sem,
    pass_sem, quad_sem, side_sem, own_sem, back_sem,
):
    rows, width = own_tokens.shape
    top = own_routes.shape[0]
    padded = gathered.shape[1]
    device = lax.axis_index("ep")
    expert = (device // 2).astype(jnp.float32)

    def other(mask):
        return device + mask * (1 - 2 * lax.rem(device // mask, 2))

    core_peer = other(1)
    side_peer = other(2)
    pair_peer = other(4)
    far_peer = other(8)
    diagonal = side_peer + pair_peer - device
    quad_peers = [None, side_peer, pair_peer, diagonal]

    peers = [core_peer, side_peer, pair_peer, diagonal, far_peer]
    barrier = pltpu.get_barrier_semaphore()
    for peer in peers:
        pl.semaphore_signal(
            barrier, inc=1, device_id={"ep": peer}, device_id_type=pl.DeviceIdType.MESH
        )

    inputs = [
        pltpu.make_async_copy(source, target, in_sem.at[i])
        for i, (source, target) in enumerate(
            ((tokens, own_tokens), (routes, own_routes), (gates, own_gates))
        )
    ]
    weights = [
        pltpu.make_async_copy(source.at[0], target, w_sem.at[i])
        for i, (source, target) in enumerate(((w_gate, vm_gate), (w_up, vm_up), (w_down, vm_down)))
    ]
    for copy in inputs:
        copy.start()

    block_rows = 4 * rows
    chunk_rows = 2 * block_rows
    edge = width // 128 * 128
    cuts = portions(padded, IN_SHARES)
    out_cuts = portions(padded, OUT_SHARES)
    pieces = range(len(cuts))
    out_pieces = range(len(out_cuts))

    def slot(chunk, core, q):
        return pl.ds(chunk * chunk_rows + core * block_rows + q * rows, rows)

    for copy in inputs:
        copy.wait()
    for copy in weights:
        copy.start()
    lanes = lax.broadcasted_iota(jnp.int32, (rows, padded - edge), 1) + edge
    mine = slot(0, 0, 0)
    partial[:, edge:] = jnp.zeros((2 * chunk_rows, padded - edge), jnp.bfloat16)
    gathered[mine, :edge] = own_tokens[:, :edge]
    gathered[mine, edge:] = jnp.zeros((rows, padded - edge), jnp.bfloat16)
    gathered[mine, edge:width] = own_tokens[:, edge:]
    scale = jnp.transpose(own_gates[...].astype(jnp.float32)) / 65536.0
    high = scale.astype(jnp.bfloat16).astype(jnp.float32)
    low = scale - high
    ids = jnp.transpose(own_routes[...].astype(jnp.float32))
    tail = gathered[mine, edge:].astype(jnp.float32)
    for k in range(top):
        tail = jnp.where(lanes == width + k, ids[:, k : k + 1], tail)
        tail = jnp.where(lanes == width + top + k, high[:, k : k + 1], tail)
        tail = jnp.where(lanes == width + 2 * top + k, low[:, k : k + 1], tail)
    gathered[mine, edge:] = tail.astype(jnp.bfloat16)

    with jax.named_scope("barrier"):
        pl.semaphore_wait(barrier, len(peers))

    def remote(source, target, send_sem, recv_sem, device_id):
        return pltpu.make_async_remote_copy(
            src_ref=source, dst_ref=target, send_sem=send_sem, recv_sem=recv_sem,
            device_id={"ep": device_id}, device_id_type=pl.DeviceIdType.MESH,
        )

    sizes = [0, 0]

    def launch(kind, source, target, recv_sem, peer):
        remote(source, target, sent.at[kind], recv_sem, peer).start()
        sizes[kind] += source.shape[0] * source.shape[1]

    def await_rows(buffer, count, cut, recv_sem):
        where = buffer.at[pl.ds(0, count * rows), cut[0] : cut[1]]
        remote(where, where, recv_sem, recv_sem, core_peer).wait_recv()

    def await_sent(kind):
        rows_sent = sizes[kind] // padded
        assert rows_sent * padded == sizes[kind]
        where = gathered.at[pl.ds(0, rows_sent), :]
        remote(where, where, sent.at[kind], sent.at[kind], core_peer).wait_send()

    def give(origin, chunk, core, q, piece, recv_sem, peer):
        cut = cuts[piece]
        launch(
            0, gathered.at[origin, cut[0] : cut[1]],
            gathered.at[slot(chunk, core, q), cut[0] : cut[1]], recv_sem.at[piece], peer,
        )

    def to_core(chunk, q, piece):
        give(slot(chunk, 0, q), chunk, 1, q, piece, core_sem, core_peer)

    for piece in pieces:
        give(mine, 1, 0, 0, piece, far_sem, far_peer)
        for q in (2, 1):
            give(mine, 0, 0, q, piece, near_sem, quad_peers[q])
        to_core(0, 0, piece)

    def take_near(piece):
        await_rows(gathered, 2, cuts[piece], near_sem.at[piece])
        give(slot(0, 0, 2), 0, 0, 3, piece, late_sem, side_peer)
        for q in (2, 1):
            to_core(0, q, piece)

    def take_far(piece):
        await_rows(gathered, 1, cuts[piece], far_sem.at[piece])
        for q in (3, 2, 1):
            give(slot(1, 0, 0), 1, 0, q, piece, late_sem, quad_peers[q])
        to_core(1, 0, piece)

    def take_late(piece):
        await_rows(gathered, 4, cuts[piece], late_sem.at[piece])
        to_core(0, 3, piece)
        for q in (1, 2, 3):
            to_core(1, q, piece)

    def add_products(piece):
        low_col, high_col = cuts[piece][0], min(cuts[piece][1], width)
        x = gathered[:, low_col:high_col]
        for weight, total in ((vm_gate, gate_sum), (vm_up, up_sum)):
            product = lax.dot_general(
                weight[:, low_col:high_col], x, NT, preferred_element_type=jnp.float32
            )
            total[...] = product if piece == 0 else total[...] + product

    def gate_factor():
        info = gathered[:, edge:].astype(jnp.float32)
        factor = jnp.zeros((2 * chunk_rows, 1), jnp.float32)
        for k in range(top):
            col = width - edge + k
            value = info[:, col + top : col + top + 1] + info[:, col + 2 * top : col + 2 * top + 1]
            factor += jnp.where(info[:, col : col + 1] == expert, value, 0.0)
        return factor

    def run_down(hidden, factor, piece):
        low_out, high_out = out_cuts[piece]
        for low_col, high_col in column_cuts(low_out, min(high_out, width), 512):
            y = lax.dot_general(
                hidden, vm_down[:, low_col:high_col], TN, preferred_element_type=jnp.float32
            )
            partial[:, low_col:high_col] = (y * factor).astype(jnp.bfloat16)
        for chunk in (1, 0):
            launch(
                1, partial.at[pl.ds(chunk * chunk_rows + block_rows, block_rows), low_out:high_out],
                from_core.at[pl.ds(chunk * block_rows, block_rows), low_out:high_out],
                pass_sem.at[piece], core_peer,
            )

    def chip_sum(chunk, q, piece):
        low_col, high_col = out_cuts[piece]
        mine_part = partial[slot(chunk, 0, q), low_col:high_col].astype(jnp.float32)
        where = pl.ds(chunk * block_rows + q * rows, rows)
        return mine_part + from_core[where, low_col:high_col].astype(jnp.float32)

    def give_sum(total, chunk, q, piece, recv_sem, peer):
        low_col, high_col = out_cuts[piece]
        where = pl.ds((chunk * 3 + q - 1) * rows, rows)
        to_quad[where, low_col:high_col] = total.astype(jnp.bfloat16)
        launch(
            1, to_quad.at[where, low_col:high_col], from_quad.at[where, low_col:high_col],
            recv_sem.at[piece], peer,
        )

    def got(chunk, q, piece):
        low_col, high_col = out_cuts[piece]
        return from_quad[pl.ds((chunk * 3 + q - 1) * rows, rows), low_col:high_col].astype(jnp.float32)

    def give_b(piece):
        low_col, high_col = out_cuts[piece]
        await_rows(gathered, 8, out_cuts[piece], pass_sem.at[piece])
        for q in (3, 1, 2):
            give_sum(chip_sum(1, q, piece), 1, q, piece, quad_sem, quad_peers[q])
        kept[pl.ds(rows, rows), low_col:high_col] = chip_sum(1, 0, piece)

    for piece in pieces:
        with jax.named_scope(f"near{piece}"):
            take_near(piece)
        with jax.named_scope(f"far{piece}"):
            take_far(piece)
    last = len(cuts) - 1
    with jax.named_scope("late0"):
        take_late(0)
    weights[0].wait()
    weights[1].wait()
    for piece in pieces:
        if piece < last:
            with jax.named_scope(f"late{piece + 1}"):
                take_late(piece + 1)
        with jax.named_scope(f"core{piece}"):
            await_rows(gathered, 8, cuts[piece], core_sem.at[piece])
        with jax.named_scope(f"dot{piece}"):
            if piece == last:
                factor = gate_factor()
            add_products(piece)
    with jax.named_scope("silu"):
        hidden = (jax.nn.silu(gate_sum[...]) * up_sum[...]).astype(jnp.bfloat16)
    weights[2].wait()
    for piece in out_pieces:
        with jax.named_scope(f"down{piece}"):
            run_down(hidden, factor, piece)
        if piece == GIVE_AT:
            with jax.named_scope("give1_0"):
                give_b(0)
    with jax.named_scope("give1"):
        for piece in out_pieces:
            if piece > 0 or GIVE_AT is None:
                give_b(piece)
    with jax.named_scope("give0"):
        for q, recv_sem in ((3, side_sem), (1, own_sem)):
            for piece in out_pieces:
                give_sum(chip_sum(0, q, piece), 0, q, piece, recv_sem, side_peer)
    with jax.named_scope("kept"):
        for piece in out_pieces:
            low_col, high_col = out_cuts[piece]
            kept[pl.ds(0, rows), low_col:high_col] = chip_sum(0, 0, piece)
            kept[pl.ds(2 * rows, rows), low_col:high_col] = chip_sum(0, 2, piece)
    for piece in out_pieces:
        low_col, high_col = out_cuts[piece]
        with jax.named_scope(f"far_out{piece}"):
            await_rows(gathered, 3, out_cuts[piece], quad_sem.at[piece])
            total = kept[pl.ds(rows, rows), low_col:high_col]
            total += got(1, 1, piece) + got(1, 2, piece) + got(1, 3, piece)
            to_far[:, low_col:high_col] = total.astype(jnp.bfloat16)
            launch(
                1, to_far.at[:, low_col:high_col], from_far.at[:, low_col:high_col],
                back_sem.at[piece], far_peer,
            )
    for piece in out_pieces:
        low_col, high_col = out_cuts[piece]
        with jax.named_scope(f"relay{piece}"):
            await_rows(gathered, 1, out_cuts[piece], side_sem.at[piece])
            total = kept[pl.ds(2 * rows, rows), low_col:high_col] + got(0, 3, piece)
            give_sum(total, 0, 2, piece, own_sem, pair_peer)
    with jax.named_scope("drain"):
        await_sent(0)
    for piece in out_pieces:
        low_col, high_col = out_cuts[piece]
        with jax.named_scope(f"final{piece}"):
            await_rows(gathered, 2, out_cuts[piece], own_sem.at[piece])
            total = kept[pl.ds(0, rows), low_col:high_col]
            total += got(0, 1, piece) + got(0, 2, piece)
        with jax.named_scope(f"end{piece}"):
            await_rows(gathered, 1, out_cuts[piece], back_sem.at[piece])
            total += from_far[:, low_col:high_col].astype(jnp.float32)
            high_col = min(high_col, width)
            out[:, low_col:high_col] = total[:, : high_col - low_col].astype(out.dtype)
    with jax.named_scope("drain_end"):
        await_sent(1)


GIVE_AT = None


def quad_local(tokens, routes, gate_fixed, gate_weight, up_weight, down_weight):
    rows, width = tokens.shape
    top = routes.shape[1]
    gate_weight = jnp.swapaxes(gate_weight, 1, 2)
    up_weight = jnp.swapaxes(up_weight, 1, 2)
    padded = -(-(width + 3 * top) // 128) * 128
    every = 16 * rows
    dma = pltpu.SemaphoreType.DMA
    ins, outs = dma((len(IN_SHARES),)), dma((len(OUT_SHARES),))
    anywhere = pl.BlockSpec(memory_space=pl.ANY)
    routes, gate_fixed = routes.T, gate_fixed.T
    return pl.pallas_call(
        quad_kernel,
        out_shape=pltpu.VMEM((rows, width), jnp.bfloat16),
        in_specs=[anywhere] * 6,
        out_specs=pl.BlockSpec(memory_space=pltpu.VMEM),
        scratch_shapes=[
            pltpu.VMEM(tokens.shape, jnp.bfloat16),
            pltpu.VMEM(routes.shape, jnp.int32),
            pltpu.VMEM(gate_fixed.shape, jnp.int32),
            pltpu.VMEM((every, padded), jnp.bfloat16),
            pltpu.VMEM(gate_weight.shape[1:], jnp.bfloat16),
            pltpu.VMEM(up_weight.shape[1:], jnp.bfloat16),
            pltpu.VMEM(down_weight.shape[1:], jnp.bfloat16),
            pltpu.VMEM((gate_weight.shape[1], every), jnp.float32),
            pltpu.VMEM((gate_weight.shape[1], every), jnp.float32),
            pltpu.VMEM((every, padded), jnp.bfloat16),
            pltpu.VMEM((8 * rows, padded), jnp.bfloat16),
            pltpu.VMEM((6 * rows, padded), jnp.bfloat16),
            pltpu.VMEM((6 * rows, padded), jnp.bfloat16),
            pltpu.VMEM((3 * rows, padded), jnp.float32),
            pltpu.VMEM((rows, padded), jnp.bfloat16),
            pltpu.VMEM((rows, padded), jnp.bfloat16),
            dma((3,)), dma((3,)), dma((2,)),
            ins, ins, ins, ins,
            outs, outs, outs, outs, outs,
        ],
        compiler_params=pltpu.CompilerParams(
            collective_id=0, has_side_effects=True, vmem_limit_bytes=60 * 2**20
        ),
    )(tokens, routes, gate_fixed, gate_weight, up_weight, down_weight)


def solution(mesh):
    placed = (
        P(("groups", "ep"), None),
        P(("groups", "ep"), None),
        P(("groups", "ep"), None),
        P("ep", None, None),
        P("ep", None, None),
        P("ep", None, None),
    )
    chips = mesh.shape["ep"] // 2

    def body(*args):
        if chips == 2**3:
            return quad_local(*args)
        return local(*args)

    return jax.shard_map(
        body, mesh=mesh, in_specs=placed, out_specs=P(("groups", "ep"), None), check_vma=False
    )
```

```python
import jax
import jax.numpy as jnp
from jax import lax
from jax.experimental import pallas as pl
from jax.experimental.pallas import tpu as pltpu
from jax.sharding import PartitionSpec as P


def swapped(value, axis, bit):
    mask = 2**bit
    pairs = [(source, source ^ mask) for source in range(lax.axis_size(axis))]
    return lax.ppermute(value, axis, pairs)


def expert_half(expert_rows, w_gate, w_up, w_down):
    gate_part = jnp.dot(expert_rows, w_gate, preferred_element_type=jnp.float32)
    up_part = jnp.dot(expert_rows, w_up, preferred_element_type=jnp.float32)
    hidden = (jax.nn.silu(gate_part) * up_part).astype(jnp.bfloat16)
    return jnp.dot(hidden, w_down, preferred_element_type=jnp.float32).astype(jnp.bfloat16)


def local(tokens, routes, gate_fixed, gate_weight, up_weight, down_weight):
    devices_ep = lax.axis_size("ep")
    experts = devices_ep // 2
    tok_count = tokens.shape[0]
    top_count = routes.shape[1]
    width = tokens.shape[1]
    capacity = 2 * tok_count * top_count // experts
    onehot = (routes[:, :, None] == jnp.arange(experts, dtype=jnp.int32)).astype(jnp.int32)
    flat_hot = onehot.reshape(tok_count * top_count, experts)
    before = jnp.cumsum(flat_hot, axis=0) - flat_hot
    position = jnp.sum(before * flat_hot, axis=1).reshape(tok_count, top_count)
    slot_index = routes * capacity + position
    select = (slot_index[:, :, None] == jnp.arange(experts * capacity, dtype=jnp.int32)).astype(
        jnp.int32
    )
    select = jnp.sum(select, axis=1).astype(jnp.bfloat16)
    packed = jnp.einsum("ts,td->sd", select, tokens, preferred_element_type=jnp.float32).astype(
        jnp.bfloat16
    )
    packed = packed.reshape(experts, 1, capacity, width)
    outgoing = jnp.broadcast_to(packed, (experts, 2, capacity, width)).reshape(
        devices_ep, capacity, width
    )
    received = lax.all_to_all(outgoing, "ep", split_axis=0, concat_axis=0, tiled=True)
    result = expert_half(received.reshape(-1, width), gate_weight[0], up_weight[0], down_weight[0])
    partial_value = result.reshape(received.shape[0], received.shape[1], width)
    parity = lax.axis_index("ep") % 2
    halves = partial_value.reshape(devices_ep, capacity, 2, width // 2)
    kept_half = lax.dynamic_index_in_dim(halves, parity, 2, keepdims=False)
    given_half = lax.dynamic_index_in_dim(halves, 1 - parity, 2, keepdims=False)
    partner = swapped(given_half, "ep", 0)
    reduced = (kept_half.astype(jnp.float32) + partner.astype(jnp.float32)).astype(jnp.bfloat16)
    returned = lax.all_to_all(reduced, "ep", split_axis=0, concat_axis=0, tiled=True)
    ordered = returned.reshape(experts, 2, capacity, width // 2).transpose(0, 2, 1, 3)
    expert_out = ordered.reshape(experts * capacity, width)
    picked = jnp.take(expert_out, slot_index.reshape(-1), axis=0).reshape(
        tok_count, top_count, width
    )
    weights = gate_fixed.astype(jnp.float32) / 65536.0
    mixed = jnp.sum(weights[:, :, None] * picked.astype(jnp.float32), axis=1)
    return mixed.astype(jnp.bfloat16)


NT = (((1,), (1,)), ((), ()))
TN = (((0,), (0,)), ((), ()))


def column_cuts(low, high, step):
    return [(start, min(start + step, high)) for start in range(low, high, step)]


def portions(padded, shares):
    tiles = padded // 128
    ends = [tiles * sum(shares[:i]) // sum(shares) * 128 for i in range(len(shares) + 1)]
    return list(zip(ends[:-1], ends[1:]))


NT = (((1,), (1,)), ((), ()))
TN = (((0,), (0,)), ((), ()))
IN_SHARES = (6, 6, 4, 7)
OUT_SHARES = (8, 8, 7)
GATHER = ("ZZZZ", "DDDD")
SCATTER = ("XXX", "DDD")
DIRECT = {"D": (1, 3, 2), "X": (1, 2), "Z": (2, 1)}
VIA = {"X": 1, "Z": 2}


def quad_kernel(
    tokens, routes, gates, w_gate, w_up, w_down, out,
    own_tokens, own_routes, own_gates, gathered, vm_gate, vm_up, vm_down, gate_sum, up_sum, partial,
    from_core, to_quad, from_quad, to_far, from_far,
    in_sem, w_sem, sent, near_sem, far_sem, mid_sem, late_sem, core_sem,
    pass_sem, hop_sem, quad_sem, own_sem, back_sem,
):
    rows, width = own_tokens.shape
    top = own_routes.shape[0]
    padded = gathered.shape[1]
    device = lax.axis_index("ep")
    expert = (device // 2).astype(jnp.float32)

    def other(mask):
        return device + mask * (1 - 2 * lax.rem(device // mask, 2))

    core_peer = other(1)
    side_peer = other(2)
    pair_peer = other(4)
    far_peer = other(8)
    diagonal = side_peer + pair_peer - device
    quad_peers = [None, side_peer, pair_peer, diagonal]

    peers = [core_peer, side_peer, pair_peer, far_peer]
    barrier = pltpu.get_barrier_semaphore()
    for peer in peers:
        pl.semaphore_signal(
            barrier, inc=1, device_id={"ep": peer}, device_id_type=pl.DeviceIdType.MESH
        )

    inputs = [
        pltpu.make_async_copy(source, target, in_sem.at[i])
        for i, (source, target) in enumerate(
            ((tokens, own_tokens), (routes, own_routes), (gates, own_gates))
        )
    ]
    weights = [
        pltpu.make_async_copy(source.at[0], target, w_sem.at[i])
        for i, (source, target) in enumerate(((w_gate, vm_gate), (w_up, vm_up), (w_down, vm_down)))
    ]
    for copy in inputs:
        copy.start()

    block_rows = 4 * rows
    chunk_rows = 2 * block_rows
    edge = width // 128 * 128
    cuts = portions(padded, IN_SHARES)
    cuts = cuts[-TURN:] + cuts[:-TURN]
    out_cuts = portions(padded, OUT_SHARES)
    pieces = range(len(cuts))
    out_pieces = range(len(out_cuts))

    def slot(chunk, core, q):
        return pl.ds(chunk * chunk_rows + core * block_rows + q * rows, rows)

    for copy in inputs:
        copy.wait()
    for copy in weights:
        copy.start()
    lanes = lax.broadcasted_iota(jnp.int32, (rows, padded - edge), 1) + edge
    mine = slot(0, 0, 0)
    partial[:, edge:] = jnp.zeros((2 * chunk_rows, padded - edge), jnp.bfloat16)
    gathered[mine, :edge] = own_tokens[:, :edge]
    gathered[mine, edge:] = jnp.zeros((rows, padded - edge), jnp.bfloat16)
    gathered[mine, edge:width] = own_tokens[:, edge:]
    scale = jnp.transpose(own_gates[...].astype(jnp.float32)) / 65536.0
    high = scale.astype(jnp.bfloat16).astype(jnp.float32)
    low = scale - high
    ids = jnp.transpose(own_routes[...].astype(jnp.float32))
    tail = gathered[mine, edge:].astype(jnp.float32)
    for k in range(top):
        tail = jnp.where(lanes == width + k, ids[:, k : k + 1], tail)
        tail = jnp.where(lanes == width + top + k, high[:, k : k + 1], tail)
        tail = jnp.where(lanes == width + 2 * top + k, low[:, k : k + 1], tail)
    gathered[mine, edge:] = tail.astype(jnp.bfloat16)

    with jax.named_scope("barrier"):
        pl.semaphore_wait(barrier, len(peers))

    def remote(source, target, send_sem, recv_sem, device_id):
        return pltpu.make_async_remote_copy(
            src_ref=source, dst_ref=target, send_sem=send_sem, recv_sem=recv_sem,
            device_id={"ep": device_id}, device_id_type=pl.DeviceIdType.MESH,
        )

    sizes = [0, 0]

    def launch(kind, source, target, recv_sem, peer):
        remote(source, target, sent.at[kind], recv_sem, peer).start()
        sizes[kind] += source.shape[0] * source.shape[1]

    def await_rows(buffer, count, cut, recv_sem):
        where = buffer.at[pl.ds(0, count * rows), cut[0] : cut[1]]
        remote(where, where, recv_sem, recv_sem, core_peer).wait_recv()

    def await_sent(kind):
        rows_sent = sizes[kind] // padded
        assert rows_sent * padded == sizes[kind]
        where = gathered.at[pl.ds(0, rows_sent), :]
        remote(where, where, sent.at[kind], sent.at[kind], core_peer).wait_send()

    def give(origin, chunk, core, q, piece, recv_sem, peer):
        cut = cuts[piece]
        launch(
            0, gathered.at[origin, cut[0] : cut[1]],
            gathered.at[slot(chunk, core, q), cut[0] : cut[1]], recv_sem.at[piece], peer,
        )

    def to_core(chunk, q, piece):
        give(slot(chunk, 0, q), chunk, 1, q, piece, core_sem, core_peer)

    def spread(chunk, piece):
        mode = GATHER[chunk][piece]
        for q in DIRECT[mode]:
            if chunk == 0 and q < 3:
                recv_sem = near_sem
            elif chunk == 1 and q == VIA.get(mode):
                recv_sem = mid_sem
            else:
                recv_sem = late_sem
            give(slot(chunk, 0, 0), chunk, 0, q, piece, recv_sem, quad_peers[q])
        to_core(chunk, 0, piece)

    def relay(chunk, piece):
        mode = GATHER[chunk][piece]
        if mode != "D":
            q = VIA[mode]
            give(slot(chunk, 0, q), chunk, 0, 3, piece, late_sem, quad_peers[3 - q])

    for piece in pieces:
        give(mine, 1, 0, 0, piece, far_sem, far_peer)
        spread(0, piece)

    def take_near(piece):
        await_rows(gathered, 2, cuts[piece], near_sem.at[piece])
        relay(0, piece)
        for q in (2, 1):
            to_core(0, q, piece)

    def take_far(piece):
        await_rows(gathered, 1, cuts[piece], far_sem.at[piece])
        spread(1, piece)

    def take_mid(piece):
        mode = GATHER[1][piece]
        if mode != "D":
            await_rows(gathered, 1, cuts[piece], mid_sem.at[piece])
            relay(1, piece)
            to_core(1, VIA[mode], piece)

    def take_late(piece):
        mode = GATHER[1][piece]
        rest = [q for q in (1, 2, 3) if q != VIA.get(mode)]
        await_rows(gathered, 1 + len(rest), cuts[piece], late_sem.at[piece])
        to_core(0, 3, piece)
        for q in rest:
            to_core(1, q, piece)

    def add_products(piece):
        low_col, high_col = cuts[piece][0], min(cuts[piece][1], width)
        x = gathered[:, low_col:high_col]
        for weight, total in ((vm_gate, gate_sum), (vm_up, up_sum)):
            product = lax.dot_general(
                weight[:, low_col:high_col], x, NT, preferred_element_type=jnp.float32
            )
            total[...] = product if piece == 0 else total[...] + product

    def gate_factor():
        info = gathered[:, edge:].astype(jnp.float32)
        factor = jnp.zeros((2 * chunk_rows, 1), jnp.float32)
        for k in range(top):
            col = width - edge + k
            value = info[:, col + top : col + top + 1] + info[:, col + 2 * top : col + 2 * top + 1]
            factor += jnp.where(info[:, col : col + 1] == expert, value, 0.0)
        return factor

    def run_down(hidden, factor, chunk, piece):
        low_out, high_out = out_cuts[piece]
        low_row = chunk * chunk_rows
        high_row = low_row + chunk_rows
        for low_col, high_col in column_cuts(low_out, min(high_out, width), BLOCK):
            y = lax.dot_general(
                hidden[:, low_row:high_row], vm_down[:, low_col:high_col], TN,
                preferred_element_type=jnp.float32,
            )
            part = (y * factor[low_row:high_row]).astype(jnp.bfloat16)
            partial[low_row:high_row, low_col:high_col] = part
        launch(
            1, partial.at[pl.ds(low_row + block_rows, block_rows), low_out:high_out],
            from_core.at[pl.ds(chunk * block_rows, block_rows), low_out:high_out],
            pass_sem.at[chunk, piece], core_peer,
        )

    def chip_sum(chunk, q, piece):
        low_col, high_col = out_cuts[piece]
        mine_part = partial[slot(chunk, 0, q), low_col:high_col].astype(jnp.float32)
        where = pl.ds(chunk * block_rows + q * rows, rows)
        return mine_part + from_core[where, low_col:high_col].astype(jnp.float32)

    def give_sum(total, chunk, q, piece, recv_sem, peer):
        low_col, high_col = out_cuts[piece]
        where = pl.ds((chunk * 3 + q - 1) * rows, rows)
        to_quad[where, low_col:high_col] = total.astype(jnp.bfloat16)
        launch(
            1, to_quad.at[where, low_col:high_col], from_quad.at[where, low_col:high_col],
            recv_sem.at[piece], peer,
        )

    def got(chunk, q, piece):
        low_col, high_col = out_cuts[piece]
        return from_quad[pl.ds((chunk * 3 + q - 1) * rows, rows), low_col:high_col].astype(jnp.float32)

    done_sem = (own_sem, quad_sem)

    def give_out(chunk, q, piece):
        mode = SCATTER[chunk][piece]
        total = chip_sum(chunk, q, piece)
        if q == 3 and mode != "D":
            give_sum(total, chunk, 3, piece, hop_sem.at[chunk], quad_peers[VIA[mode]])
        elif mode == "D" or q == VIA[mode]:
            give_sum(total, chunk, q, piece, done_sem[chunk], quad_peers[q])

    def give_b(piece):
        await_rows(gathered, 4, out_cuts[piece], pass_sem.at[1, piece])
        for q in (3, 1, 2):
            give_out(1, q, piece)

    def relay_out(chunk, piece):
        mode = SCATTER[chunk][piece]
        if mode != "D":
            q = 3 - VIA[mode]
            await_rows(gathered, 1, out_cuts[piece], hop_sem.at[chunk, piece])
            total = chip_sum(chunk, q, piece) + got(chunk, 3, piece)
            give_sum(total, chunk, q, piece, done_sem[chunk], quad_peers[q])

    def quad_total(chunk, piece):
        direct = SCATTER[chunk][piece] == "D"
        await_rows(gathered, 3 if direct else 2, out_cuts[piece], done_sem[chunk].at[piece])
        total = chip_sum(chunk, 0, piece) + got(chunk, 1, piece) + got(chunk, 2, piece)
        return total + got(chunk, 3, piece) if direct else total

    for piece in pieces:
        with jax.named_scope(f"near{piece}"):
            take_near(piece)
        with jax.named_scope(f"far{piece}"):
            take_far(piece)
    for piece in pieces:
        with jax.named_scope(f"mid{piece}"):
            take_mid(piece)
    last = len(cuts) - 1
    def dots(piece):
        with jax.named_scope(f"core{piece}"):
            await_rows(gathered, 8, cuts[piece], core_sem.at[piece])
        with jax.named_scope(f"dot{piece}"):
            add_products(piece)

    for piece in pieces:
        with jax.named_scope(f"late{piece}"):
            take_late(piece)
        if piece == 0:
            weights[0].wait()
            weights[1].wait()
        if piece > 0:
            dots(piece - 1)
    dots(last)
    factor = gate_factor()
    with jax.named_scope("silu"):
        hidden = (jax.nn.silu(gate_sum[...]) * up_sum[...]).astype(jnp.bfloat16)
    weights[2].wait()
    with jax.named_scope("down1"):
        for piece in out_pieces:
            run_down(hidden, factor, 1, piece)
    gave = 0
    for piece in out_pieces:
        with jax.named_scope(f"down0_{piece}"):
            run_down(hidden, factor, 0, piece)
        if piece >= GIVE_AT:
            with jax.named_scope(f"give1_{gave}"):
                give_b(gave)
            gave += 1
    for piece in list(out_pieces)[gave:]:
        with jax.named_scope(f"give1_{piece}"):
            give_b(piece)
    for piece in out_pieces:
        await_rows(gathered, 4, out_cuts[piece], pass_sem.at[0, piece])
    with jax.named_scope("give0"):
        for q in (3, 1):
            for piece in out_pieces:
                give_out(0, q, piece)

    def far_out(piece):
        low_col, high_col = out_cuts[piece]
        to_far[:, low_col:high_col] = quad_total(1, piece).astype(jnp.bfloat16)
        launch(
            1, to_far.at[:, low_col:high_col], from_far.at[:, low_col:high_col],
            back_sem.at[piece], far_peer,
        )

    for kind, piece in PLAN:
        with jax.named_scope(f"{kind}{piece}"):
            if kind == "hop":
                relay_out(0, piece)
            else:
                far_out(piece)
    with jax.named_scope("drain"):
        await_sent(0)
    for piece in out_pieces:
        low_col, high_col = out_cuts[piece]
        with jax.named_scope(f"final{piece}"):
            total = quad_total(0, piece)
        with jax.named_scope(f"end{piece}"):
            await_rows(gathered, 1, out_cuts[piece], back_sem.at[piece])
            total += from_far[:, low_col:high_col].astype(jnp.float32)
            high_col = min(high_col, width)
            out[:, low_col:high_col] = total[:, : high_col - low_col].astype(out.dtype)
    with jax.named_scope("drain_end"):
        await_sent(1)


GIVE_AT = 0
PLAN = (("far", 0), ("far", 1), ("hop", 0), ("far", 2), ("hop", 1), ("hop", 2))
TURN = 1
BLOCK = 1024


def quad_local(tokens, routes, gate_fixed, gate_weight, up_weight, down_weight):
    rows, width = tokens.shape
    top = routes.shape[1]
    gate_weight = jnp.swapaxes(gate_weight, 1, 2)
    up_weight = jnp.swapaxes(up_weight, 1, 2)
    padded = -(-(width + 3 * top) // 128) * 128
    every = 16 * rows
    dma = pltpu.SemaphoreType.DMA
    ins, outs = dma((len(IN_SHARES),)), dma((len(OUT_SHARES),))
    anywhere = pl.BlockSpec(memory_space=pl.ANY)
    routes, gate_fixed = routes.T, gate_fixed.T
    return pl.pallas_call(
        quad_kernel,
        out_shape=pltpu.VMEM((rows, width), jnp.bfloat16),
        in_specs=[anywhere] * 6,
        out_specs=pl.BlockSpec(memory_space=pltpu.VMEM),
        scratch_shapes=[
            pltpu.VMEM(tokens.shape, jnp.bfloat16),
            pltpu.VMEM(routes.shape, jnp.int32),
            pltpu.VMEM(gate_fixed.shape, jnp.int32),
            pltpu.VMEM((every, padded), jnp.bfloat16),
            pltpu.VMEM(gate_weight.shape[1:], jnp.bfloat16),
            pltpu.VMEM(up_weight.shape[1:], jnp.bfloat16),
            pltpu.VMEM(down_weight.shape[1:], jnp.bfloat16),
            pltpu.VMEM((gate_weight.shape[1], every), jnp.float32),
            pltpu.VMEM((gate_weight.shape[1], every), jnp.float32),
            pltpu.VMEM((every, padded), jnp.bfloat16),
            pltpu.VMEM((8 * rows, padded), jnp.bfloat16),
            pltpu.VMEM((6 * rows, padded), jnp.bfloat16),
            pltpu.VMEM((6 * rows, padded), jnp.bfloat16),
            pltpu.VMEM((rows, padded), jnp.bfloat16),
            pltpu.VMEM((rows, padded), jnp.bfloat16),
            dma((3,)), dma((3,)), dma((2,)),
            ins, ins, ins, ins, ins,
            dma((2, len(OUT_SHARES))), dma((2, len(OUT_SHARES))), outs, outs, outs,
        ],
        compiler_params=pltpu.CompilerParams(
            collective_id=0, has_side_effects=True, vmem_limit_bytes=60 * 2**20
        ),
    )(tokens, routes, gate_fixed, gate_weight, up_weight, down_weight)


def solution(mesh):
    placed = (
        P(("groups", "ep"), None),
        P(("groups", "ep"), None),
        P(("groups", "ep"), None),
        P("ep", None, None),
        P("ep", None, None),
        P("ep", None, None),
    )
    chips = mesh.shape["ep"] // 2

    def body(*args):
        if chips == 2**3:
            return quad_local(*args)
        return local(*args)

    return jax.shard_map(
        body, mesh=mesh, in_specs=placed, out_specs=P(("groups", "ep"), None), check_vma=False
    )
```

```python
import jax
import jax.numpy as jnp
from jax import lax
from jax.experimental import pallas as pl
from jax.experimental.pallas import tpu as pltpu
from jax.sharding import PartitionSpec as P


def swapped(value, axis, bit):
    mask = 2**bit
    pairs = [(source, source ^ mask) for source in range(lax.axis_size(axis))]
    return lax.ppermute(value, axis, pairs)


def expert_half(expert_rows, w_gate, w_up, w_down):
    gate_part = jnp.dot(expert_rows, w_gate, preferred_element_type=jnp.float32)
    up_part = jnp.dot(expert_rows, w_up, preferred_element_type=jnp.float32)
    hidden = (jax.nn.silu(gate_part) * up_part).astype(jnp.bfloat16)
    return jnp.dot(hidden, w_down, preferred_element_type=jnp.float32).astype(jnp.bfloat16)


def local(tokens, routes, gate_fixed, gate_weight, up_weight, down_weight):
    devices_ep = lax.axis_size("ep")
    experts = devices_ep // 2
    tok_count = tokens.shape[0]
    top_count = routes.shape[1]
    width = tokens.shape[1]
    capacity = 2 * tok_count * top_count // experts
    onehot = (routes[:, :, None] == jnp.arange(experts, dtype=jnp.int32)).astype(jnp.int32)
    flat_hot = onehot.reshape(tok_count * top_count, experts)
    before = jnp.cumsum(flat_hot, axis=0) - flat_hot
    position = jnp.sum(before * flat_hot, axis=1).reshape(tok_count, top_count)
    slot_index = routes * capacity + position
    select = (slot_index[:, :, None] == jnp.arange(experts * capacity, dtype=jnp.int32)).astype(
        jnp.int32
    )
    select = jnp.sum(select, axis=1).astype(jnp.bfloat16)
    packed = jnp.einsum("ts,td->sd", select, tokens, preferred_element_type=jnp.float32).astype(
        jnp.bfloat16
    )
    packed = packed.reshape(experts, 1, capacity, width)
    outgoing = jnp.broadcast_to(packed, (experts, 2, capacity, width)).reshape(
        devices_ep, capacity, width
    )
    received = lax.all_to_all(outgoing, "ep", split_axis=0, concat_axis=0, tiled=True)
    result = expert_half(received.reshape(-1, width), gate_weight[0], up_weight[0], down_weight[0])
    partial_value = result.reshape(received.shape[0], received.shape[1], width)
    parity = lax.axis_index("ep") % 2
    halves = partial_value.reshape(devices_ep, capacity, 2, width // 2)
    kept_half = lax.dynamic_index_in_dim(halves, parity, 2, keepdims=False)
    given_half = lax.dynamic_index_in_dim(halves, 1 - parity, 2, keepdims=False)
    partner = swapped(given_half, "ep", 0)
    reduced = (kept_half.astype(jnp.float32) + partner.astype(jnp.float32)).astype(jnp.bfloat16)
    returned = lax.all_to_all(reduced, "ep", split_axis=0, concat_axis=0, tiled=True)
    ordered = returned.reshape(experts, 2, capacity, width // 2).transpose(0, 2, 1, 3)
    expert_out = ordered.reshape(experts * capacity, width)
    picked = jnp.take(expert_out, slot_index.reshape(-1), axis=0).reshape(
        tok_count, top_count, width
    )
    weights = gate_fixed.astype(jnp.float32) / 65536.0
    mixed = jnp.sum(weights[:, :, None] * picked.astype(jnp.float32), axis=1)
    return mixed.astype(jnp.bfloat16)


NT = (((1,), (1,)), ((), ()))
TN = (((0,), (0,)), ((), ()))


def column_cuts(low, high, step):
    return [(start, min(start + step, high)) for start in range(low, high, step)]


def portions(padded, shares):
    tiles = padded // 128
    ends = [tiles * sum(shares[:i]) // sum(shares) * 128 for i in range(len(shares) + 1)]
    return list(zip(ends[:-1], ends[1:]))


NT = (((1,), (1,)), ((), ()))
TN = (((0,), (0,)), ((), ()))
IN_SHARES = (6, 6, 4, 7)
OUT_SHARES = (8, 8, 7)
GATHER = ("ZZXZ", "DDDD")
SCATTER = ("XXX", "DDD")
DIRECT = {"D": (1, 3, 2), "X": (1, 2), "Z": (2, 1)}
VIA = {"X": 1, "Z": 2}


def quad_kernel(
    tokens, routes, gates, w_gate, w_up, w_down, out,
    own_tokens, own_routes, own_gates, gathered, vm_gate, vm_up, vm_down, gate_sum, up_sum, partial,
    from_core, to_quad, from_quad, to_far, from_far,
    in_sem, w_sem, sent, near_sem, far_sem, mid_sem, late_sem, core_sem,
    pass_sem, hop_sem, quad_sem, own_sem, back_sem,
):
    rows, width = own_tokens.shape
    top = own_routes.shape[0]
    padded = gathered.shape[1]
    device = lax.axis_index("ep")
    expert = (device // 2).astype(jnp.float32)

    def other(mask):
        return device + mask * (1 - 2 * lax.rem(device // mask, 2))

    core_peer = other(1)
    side_peer = other(2)
    pair_peer = other(4)
    far_peer = other(8)
    diagonal = side_peer + pair_peer - device
    quad_peers = [None, side_peer, pair_peer, diagonal]

    peers = [core_peer, side_peer, pair_peer, far_peer]
    barrier = pltpu.get_barrier_semaphore()
    for peer in peers:
        pl.semaphore_signal(
            barrier, inc=1, device_id={"ep": peer}, device_id_type=pl.DeviceIdType.MESH
        )

    inputs = [
        pltpu.make_async_copy(source, target, in_sem.at[i])
        for i, (source, target) in enumerate(
            ((tokens, own_tokens), (routes, own_routes), (gates, own_gates))
        )
    ]
    weights = [
        pltpu.make_async_copy(source.at[0], target, w_sem.at[i])
        for i, (source, target) in enumerate(((w_gate, vm_gate), (w_up, vm_up), (w_down, vm_down)))
    ]
    for copy in inputs:
        copy.start()

    block_rows = 4 * rows
    chunk_rows = 2 * block_rows
    edge = width // 128 * 128
    cuts = portions(padded, IN_SHARES)
    cuts = cuts[-TURN:] + cuts[:-TURN]
    out_cuts = portions(padded, OUT_SHARES)
    pieces = range(len(cuts))
    out_pieces = range(len(out_cuts))

    def slot(chunk, core, q):
        return pl.ds(chunk * chunk_rows + core * block_rows + q * rows, rows)

    for copy in inputs:
        copy.wait()
    for copy in weights:
        copy.start()
    lanes = lax.broadcasted_iota(jnp.int32, (rows, padded - edge), 1) + edge
    mine = slot(0, 0, 0)
    partial[:, edge:] = jnp.zeros((2 * chunk_rows, padded - edge), jnp.bfloat16)
    gathered[mine, :edge] = own_tokens[:, :edge]
    gathered[mine, edge:] = jnp.zeros((rows, padded - edge), jnp.bfloat16)
    gathered[mine, edge:width] = own_tokens[:, edge:]
    scale = jnp.transpose(own_gates[...].astype(jnp.float32)) / 65536.0
    high = scale.astype(jnp.bfloat16).astype(jnp.float32)
    low = scale - high
    ids = jnp.transpose(own_routes[...].astype(jnp.float32))
    tail = gathered[mine, edge:].astype(jnp.float32)
    for k in range(top):
        tail = jnp.where(lanes == width + k, ids[:, k : k + 1], tail)
        tail = jnp.where(lanes == width + top + k, high[:, k : k + 1], tail)
        tail = jnp.where(lanes == width + 2 * top + k, low[:, k : k + 1], tail)
    gathered[mine, edge:] = tail.astype(jnp.bfloat16)

    with jax.named_scope("barrier"):
        pl.semaphore_wait(barrier, len(peers))

    def remote(source, target, send_sem, recv_sem, device_id):
        return pltpu.make_async_remote_copy(
            src_ref=source, dst_ref=target, send_sem=send_sem, recv_sem=recv_sem,
            device_id={"ep": device_id}, device_id_type=pl.DeviceIdType.MESH,
        )

    sizes = [0, 0]

    def launch(kind, source, target, recv_sem, peer):
        remote(source, target, sent.at[kind], recv_sem, peer).start()
        sizes[kind] += source.shape[0] * source.shape[1]

    def await_rows(buffer, count, cut, recv_sem):
        where = buffer.at[pl.ds(0, count * rows), cut[0] : cut[1]]
        remote(where, where, recv_sem, recv_sem, core_peer).wait_recv()

    def await_sent(kind):
        rows_sent = sizes[kind] // padded
        assert rows_sent * padded == sizes[kind]
        where = gathered.at[pl.ds(0, rows_sent), :]
        remote(where, where, sent.at[kind], sent.at[kind], core_peer).wait_send()

    def give(origin, chunk, core, q, piece, recv_sem, peer):
        cut = cuts[piece]
        launch(
            0, gathered.at[origin, cut[0] : cut[1]],
            gathered.at[slot(chunk, core, q), cut[0] : cut[1]], recv_sem.at[piece], peer,
        )

    def to_core(chunk, q, piece):
        give(slot(chunk, 0, q), chunk, 1, q, piece, core_sem, core_peer)

    def spread(chunk, piece):
        mode = GATHER[chunk][piece]
        for q in DIRECT[mode]:
            if chunk == 0 and q < 3:
                recv_sem = near_sem
            elif chunk == 1 and q == VIA.get(mode):
                recv_sem = mid_sem
            else:
                recv_sem = late_sem
            give(slot(chunk, 0, 0), chunk, 0, q, piece, recv_sem, quad_peers[q])
        to_core(chunk, 0, piece)

    def relay(chunk, piece):
        mode = GATHER[chunk][piece]
        if mode != "D":
            q = VIA[mode]
            give(slot(chunk, 0, q), chunk, 0, 3, piece, late_sem, quad_peers[3 - q])

    for piece in pieces:
        give(mine, 1, 0, 0, piece, far_sem, far_peer)
        spread(0, piece)

    def take_near(piece):
        await_rows(gathered, 2, cuts[piece], near_sem.at[piece])
        relay(0, piece)
        for q in (2, 1):
            to_core(0, q, piece)

    def take_far(piece):
        await_rows(gathered, 1, cuts[piece], far_sem.at[piece])
        spread(1, piece)

    def take_mid(piece):
        mode = GATHER[1][piece]
        if mode != "D":
            await_rows(gathered, 1, cuts[piece], mid_sem.at[piece])
            relay(1, piece)
            to_core(1, VIA[mode], piece)

    def take_late(piece):
        mode = GATHER[1][piece]
        rest = [q for q in (1, 2, 3) if q != VIA.get(mode)]
        await_rows(gathered, 1 + len(rest), cuts[piece], late_sem.at[piece])
        to_core(0, 3, piece)
        for q in rest:
            to_core(1, q, piece)

    def add_products(piece):
        low_col, high_col = cuts[piece][0], min(cuts[piece][1], width)
        x = gathered[:, low_col:high_col]
        for weight, total in ((vm_gate, gate_sum), (vm_up, up_sum)):
            product = lax.dot_general(
                weight[:, low_col:high_col], x, NT, preferred_element_type=jnp.float32
            )
            total[...] = product if piece == 0 else total[...] + product

    def gate_factor():
        info = gathered[:, edge:].astype(jnp.float32)
        factor = jnp.zeros((2 * chunk_rows, 1), jnp.float32)
        for k in range(top):
            col = width - edge + k
            value = info[:, col + top : col + top + 1] + info[:, col + 2 * top : col + 2 * top + 1]
            factor += jnp.where(info[:, col : col + 1] == expert, value, 0.0)
        return factor

    def run_down(hidden, factor, chunk, piece):
        low_out, high_out = out_cuts[piece]
        low_row = chunk * chunk_rows
        high_row = low_row + chunk_rows
        for low_col, high_col in column_cuts(low_out, min(high_out, width), BLOCK):
            y = lax.dot_general(
                hidden[:, low_row:high_row], vm_down[:, low_col:high_col], TN,
                preferred_element_type=jnp.float32,
            )
            part = (y * factor[low_row:high_row]).astype(jnp.bfloat16)
            partial[low_row:high_row, low_col:high_col] = part
        launch(
            1, partial.at[pl.ds(low_row + block_rows, block_rows), low_out:high_out],
            from_core.at[pl.ds(chunk * block_rows, block_rows), low_out:high_out],
            pass_sem.at[chunk, piece], core_peer,
        )

    def chip_sum(chunk, q, piece):
        low_col, high_col = out_cuts[piece]
        mine_part = partial[slot(chunk, 0, q), low_col:high_col].astype(jnp.float32)
        where = pl.ds(chunk * block_rows + q * rows, rows)
        return mine_part + from_core[where, low_col:high_col].astype(jnp.float32)

    def give_sum(total, chunk, q, piece, recv_sem, peer):
        low_col, high_col = out_cuts[piece]
        where = pl.ds((chunk * 3 + q - 1) * rows, rows)
        to_quad[where, low_col:high_col] = total.astype(jnp.bfloat16)
        launch(
            1, to_quad.at[where, low_col:high_col], from_quad.at[where, low_col:high_col],
            recv_sem.at[piece], peer,
        )

    def got(chunk, q, piece):
        low_col, high_col = out_cuts[piece]
        return from_quad[pl.ds((chunk * 3 + q - 1) * rows, rows), low_col:high_col].astype(jnp.float32)

    done_sem = (own_sem, quad_sem)

    def give_out(chunk, q, piece):
        mode = SCATTER[chunk][piece]
        total = chip_sum(chunk, q, piece)
        if q == 3 and mode != "D":
            give_sum(total, chunk, 3, piece, hop_sem.at[chunk], quad_peers[VIA[mode]])
        elif mode == "D" or q == VIA[mode]:
            give_sum(total, chunk, q, piece, done_sem[chunk], quad_peers[q])

    def give_b(piece):
        await_rows(gathered, 4, out_cuts[piece], pass_sem.at[1, piece])
        for q in (3, 1, 2):
            give_out(1, q, piece)

    def relay_out(chunk, piece):
        mode = SCATTER[chunk][piece]
        if mode != "D":
            q = 3 - VIA[mode]
            await_rows(gathered, 1, out_cuts[piece], hop_sem.at[chunk, piece])
            total = chip_sum(chunk, q, piece) + got(chunk, 3, piece)
            give_sum(total, chunk, q, piece, done_sem[chunk], quad_peers[q])

    def quad_total(chunk, piece):
        direct = SCATTER[chunk][piece] == "D"
        await_rows(gathered, 3 if direct else 2, out_cuts[piece], done_sem[chunk].at[piece])
        total = chip_sum(chunk, 0, piece) + got(chunk, 1, piece) + got(chunk, 2, piece)
        return total + got(chunk, 3, piece) if direct else total

    for piece in pieces:
        with jax.named_scope(f"near{piece}"):
            take_near(piece)
        with jax.named_scope(f"far{piece}"):
            take_far(piece)
    for piece in pieces:
        with jax.named_scope(f"mid{piece}"):
            take_mid(piece)
    last = len(cuts) - 1
    def dots(piece):
        with jax.named_scope(f"core{piece}"):
            await_rows(gathered, 8, cuts[piece], core_sem.at[piece])
        with jax.named_scope(f"dot{piece}"):
            add_products(piece)

    for kind, piece in STEPS:
        if kind == "late":
            with jax.named_scope(f"late{piece}"):
                take_late(piece)
            continue
        if piece == 0:
            weights[0].wait()
            weights[1].wait()
        if piece == FACTOR:
            with jax.named_scope("factor"):
                factor = gate_factor()
        dots(piece)
    with jax.named_scope("silu"):
        hidden = (jax.nn.silu(gate_sum[...]) * up_sum[...]).astype(jnp.bfloat16)
    weights[2].wait()
    with jax.named_scope("down1"):
        for piece in out_pieces:
            run_down(hidden, factor, 1, piece)
    gave = 0
    for piece in out_pieces:
        with jax.named_scope(f"down0_{piece}"):
            run_down(hidden, factor, 0, piece)
        if piece >= GIVE_AT:
            with jax.named_scope(f"give1_{gave}"):
                give_b(gave)
            gave += 1
    for piece in list(out_pieces)[gave:]:
        with jax.named_scope(f"give1_{piece}"):
            give_b(piece)
    for piece in out_pieces:
        await_rows(gathered, 4, out_cuts[piece], pass_sem.at[0, piece])
    with jax.named_scope("give0"):
        for q in (3, 1):
            for piece in out_pieces:
                give_out(0, q, piece)

    def far_out(piece):
        low_col, high_col = out_cuts[piece]
        to_far[:, low_col:high_col] = quad_total(1, piece).astype(jnp.bfloat16)
        launch(
            1, to_far.at[:, low_col:high_col], from_far.at[:, low_col:high_col],
            back_sem.at[piece], far_peer,
        )

    for kind, piece in PLAN:
        with jax.named_scope(f"{kind}{piece}"):
            if kind == "hop":
                relay_out(0, piece)
            elif kind == "pair":
                give_out(0, 2, piece)
            else:
                far_out(piece)
    with jax.named_scope("drain"):
        await_sent(0)
    for piece in out_pieces:
        low_col, high_col = out_cuts[piece]
        with jax.named_scope(f"final{piece}"):
            total = quad_total(0, piece)
        with jax.named_scope(f"end{piece}"):
            await_rows(gathered, 1, out_cuts[piece], back_sem.at[piece])
            total += from_far[:, low_col:high_col].astype(jnp.float32)
            high_col = min(high_col, width)
            out[:, low_col:high_col] = total[:, : high_col - low_col].astype(out.dtype)
    with jax.named_scope("drain_end"):
        await_sent(1)


GIVE_AT = 0
PLAN = (("far", 0), ("far", 1), ("hop", 0), ("far", 2), ("hop", 1), ("hop", 2))
TURN = 1
BLOCK = 1024
FACTOR = 2
STEPS = [("late", 0), ("late", 1), ("dot", 0), ("late", 2), ("late", 3), ("dot", 1), ("dot", 2), ("dot", 3)]


def quad_local(tokens, routes, gate_fixed, gate_weight, up_weight, down_weight):
    rows, width = tokens.shape
    top = routes.shape[1]
    gate_weight = jnp.swapaxes(gate_weight, 1, 2)
    up_weight = jnp.swapaxes(up_weight, 1, 2)
    padded = -(-(width + 3 * top) // 128) * 128
    every = 16 * rows
    dma = pltpu.SemaphoreType.DMA
    ins, outs = dma((len(IN_SHARES),)), dma((len(OUT_SHARES),))
    anywhere = pl.BlockSpec(memory_space=pl.ANY)
    routes, gate_fixed = routes.T, gate_fixed.T
    return pl.pallas_call(
        quad_kernel,
        out_shape=pltpu.VMEM((rows, width), jnp.bfloat16),
        in_specs=[anywhere] * 6,
        out_specs=pl.BlockSpec(memory_space=pltpu.VMEM),
        scratch_shapes=[
            pltpu.VMEM(tokens.shape, jnp.bfloat16),
            pltpu.VMEM(routes.shape, jnp.int32),
            pltpu.VMEM(gate_fixed.shape, jnp.int32),
            pltpu.VMEM((every, padded), jnp.bfloat16),
            pltpu.VMEM(gate_weight.shape[1:], jnp.bfloat16),
            pltpu.VMEM(up_weight.shape[1:], jnp.bfloat16),
            pltpu.VMEM(down_weight.shape[1:], jnp.bfloat16),
            pltpu.VMEM((gate_weight.shape[1], every), jnp.float32),
            pltpu.VMEM((gate_weight.shape[1], every), jnp.float32),
            pltpu.VMEM((every, padded), jnp.bfloat16),
            pltpu.VMEM((8 * rows, padded), jnp.bfloat16),
            pltpu.VMEM((6 * rows, padded), jnp.bfloat16),
            pltpu.VMEM((6 * rows, padded), jnp.bfloat16),
            pltpu.VMEM((rows, padded), jnp.bfloat16),
            pltpu.VMEM((rows, padded), jnp.bfloat16),
            dma((3,)), dma((3,)), dma((2,)),
            ins, ins, ins, ins, ins,
            dma((2, len(OUT_SHARES))), dma((2, len(OUT_SHARES))), outs, outs, outs,
        ],
        compiler_params=pltpu.CompilerParams(
            collective_id=0, has_side_effects=True, vmem_limit_bytes=60 * 2**20
        ),
    )(tokens, routes, gate_fixed, gate_weight, up_weight, down_weight)


def solution(mesh):
    placed = (
        P(("groups", "ep"), None),
        P(("groups", "ep"), None),
        P(("groups", "ep"), None),
        P("ep", None, None),
        P("ep", None, None),
        P("ep", None, None),
    )
    chips = mesh.shape["ep"] // 2

    def body(*args):
        if chips == 2**3:
            return quad_local(*args)
        return local(*args)

    return jax.shard_map(
        body, mesh=mesh, in_specs=placed, out_specs=P(("groups", "ep"), None), check_vma=False
    )
```

```python
import jax
import jax.numpy as jnp
from jax import lax
from jax.experimental import pallas as pl
from jax.experimental.pallas import tpu as pltpu
from jax.sharding import PartitionSpec as P


def swapped(value, axis, bit):
    mask = 2**bit
    pairs = [(source, source ^ mask) for source in range(lax.axis_size(axis))]
    return lax.ppermute(value, axis, pairs)


def expert_half(expert_rows, w_gate, w_up, w_down):
    gate_part = jnp.dot(expert_rows, w_gate, preferred_element_type=jnp.float32)
    up_part = jnp.dot(expert_rows, w_up, preferred_element_type=jnp.float32)
    hidden = (jax.nn.silu(gate_part) * up_part).astype(jnp.bfloat16)
    return jnp.dot(hidden, w_down, preferred_element_type=jnp.float32).astype(jnp.bfloat16)


def local(tokens, routes, gate_fixed, gate_weight, up_weight, down_weight):
    devices_ep = lax.axis_size("ep")
    experts = devices_ep // 2
    tok_count = tokens.shape[0]
    top_count = routes.shape[1]
    width = tokens.shape[1]
    capacity = 2 * tok_count * top_count // experts
    onehot = (routes[:, :, None] == jnp.arange(experts, dtype=jnp.int32)).astype(jnp.int32)
    flat_hot = onehot.reshape(tok_count * top_count, experts)
    before = jnp.cumsum(flat_hot, axis=0) - flat_hot
    position = jnp.sum(before * flat_hot, axis=1).reshape(tok_count, top_count)
    slot_index = routes * capacity + position
    select = (slot_index[:, :, None] == jnp.arange(experts * capacity, dtype=jnp.int32)).astype(
        jnp.int32
    )
    select = jnp.sum(select, axis=1).astype(jnp.bfloat16)
    packed = jnp.einsum("ts,td->sd", select, tokens, preferred_element_type=jnp.float32).astype(
        jnp.bfloat16
    )
    packed = packed.reshape(experts, 1, capacity, width)
    outgoing = jnp.broadcast_to(packed, (experts, 2, capacity, width)).reshape(
        devices_ep, capacity, width
    )
    received = lax.all_to_all(outgoing, "ep", split_axis=0, concat_axis=0, tiled=True)
    result = expert_half(received.reshape(-1, width), gate_weight[0], up_weight[0], down_weight[0])
    partial_value = result.reshape(received.shape[0], received.shape[1], width)
    parity = lax.axis_index("ep") % 2
    halves = partial_value.reshape(devices_ep, capacity, 2, width // 2)
    kept_half = lax.dynamic_index_in_dim(halves, parity, 2, keepdims=False)
    given_half = lax.dynamic_index_in_dim(halves, 1 - parity, 2, keepdims=False)
    partner = swapped(given_half, "ep", 0)
    reduced = (kept_half.astype(jnp.float32) + partner.astype(jnp.float32)).astype(jnp.bfloat16)
    returned = lax.all_to_all(reduced, "ep", split_axis=0, concat_axis=0, tiled=True)
    ordered = returned.reshape(experts, 2, capacity, width // 2).transpose(0, 2, 1, 3)
    expert_out = ordered.reshape(experts * capacity, width)
    picked = jnp.take(expert_out, slot_index.reshape(-1), axis=0).reshape(
        tok_count, top_count, width
    )
    weights = gate_fixed.astype(jnp.float32) / 65536.0
    mixed = jnp.sum(weights[:, :, None] * picked.astype(jnp.float32), axis=1)
    return mixed.astype(jnp.bfloat16)


NT = (((1,), (1,)), ((), ()))
TN = (((0,), (0,)), ((), ()))


def column_cuts(low, high, step):
    return [(start, min(start + step, high)) for start in range(low, high, step)]


def portions(padded, shares):
    tiles = padded // 128
    ends = [tiles * sum(shares[:i]) // sum(shares) * 128 for i in range(len(shares) + 1)]
    return list(zip(ends[:-1], ends[1:]))


NT = (((1,), (1,)), ((), ()))
TN = (((0,), (0,)), ((), ()))
IN_SHARES = (6, 6, 4, 7)
OUT_SHARES = (8, 8, 7)
GATHER = ("ZZXZ", "DDDD")
SCATTER = ("XXX", "DDD")
DIRECT = {"D": (1, 3, 2), "X": (1, 2), "Z": (2, 1)}
VIA = {"X": 1, "Z": 2}


def quad_kernel(
    tokens, routes, gates, w_gate, w_up, w_down, out,
    own_tokens, own_routes, own_gates, gathered, vm_gate, vm_up, vm_down, gate_sum, up_sum, partial,
    from_core, to_quad, from_quad, to_far, from_far,
    in_sem, w_sem, sent, near_sem, far_sem, mid_sem, late_sem, core_sem,
    pass_sem, hop_sem, quad_sem, own_sem, back_sem,
):
    rows, width = own_tokens.shape
    top = own_routes.shape[0]
    padded = gathered.shape[1]
    device = lax.axis_index("ep")
    expert = (device // 2).astype(jnp.float32)

    def other(mask):
        return device + mask * (1 - 2 * lax.rem(device // mask, 2))

    core_peer = other(1)
    side_peer = other(2)
    pair_peer = other(4)
    far_peer = other(8)
    diagonal = side_peer + pair_peer - device
    quad_peers = [None, side_peer, pair_peer, diagonal]

    peers = [core_peer, side_peer, pair_peer, far_peer]
    barrier = pltpu.get_barrier_semaphore()
    for peer in peers:
        pl.semaphore_signal(
            barrier, inc=1, device_id={"ep": peer}, device_id_type=pl.DeviceIdType.MESH
        )

    inputs = [
        pltpu.make_async_copy(source, target, in_sem.at[i])
        for i, (source, target) in enumerate(
            ((tokens, own_tokens), (routes, own_routes), (gates, own_gates))
        )
    ]
    weights = [
        pltpu.make_async_copy(source.at[0], target, w_sem.at[i])
        for i, (source, target) in enumerate(((w_gate, vm_gate), (w_up, vm_up), (w_down, vm_down)))
    ]
    for copy in inputs:
        copy.start()

    block_rows = 4 * rows
    chunk_rows = 2 * block_rows
    edge = width // 128 * 128
    cuts = portions(padded, IN_SHARES)
    cuts = cuts[-TURN:] + cuts[:-TURN]
    out_cuts = portions(padded, OUT_SHARES)
    pieces = range(len(cuts))
    out_pieces = range(len(out_cuts))

    def slot(chunk, core, q):
        return pl.ds(chunk * chunk_rows + core * block_rows + q * rows, rows)

    for copy in inputs:
        copy.wait()
    for copy in weights:
        copy.start()
    lanes = lax.broadcasted_iota(jnp.int32, (rows, padded - edge), 1) + edge
    mine = slot(0, 0, 0)
    partial[:, edge:] = jnp.zeros((2 * chunk_rows, padded - edge), jnp.bfloat16)
    gathered[mine, :edge] = own_tokens[:, :edge]
    gathered[mine, edge:] = jnp.zeros((rows, padded - edge), jnp.bfloat16)
    gathered[mine, edge:width] = own_tokens[:, edge:]
    scale = jnp.transpose(own_gates[...].astype(jnp.float32)) / 65536.0
    high = scale.astype(jnp.bfloat16).astype(jnp.float32)
    low = scale - high
    ids = jnp.transpose(own_routes[...].astype(jnp.float32))
    tail = gathered[mine, edge:].astype(jnp.float32)
    for k in range(top):
        tail = jnp.where(lanes == width + k, ids[:, k : k + 1], tail)
        tail = jnp.where(lanes == width + top + k, high[:, k : k + 1], tail)
        tail = jnp.where(lanes == width + 2 * top + k, low[:, k : k + 1], tail)
    gathered[mine, edge:] = tail.astype(jnp.bfloat16)

    with jax.named_scope("barrier"):
        pl.semaphore_wait(barrier, len(peers))

    def remote(source, target, send_sem, recv_sem, device_id):
        return pltpu.make_async_remote_copy(
            src_ref=source, dst_ref=target, send_sem=send_sem, recv_sem=recv_sem,
            device_id={"ep": device_id}, device_id_type=pl.DeviceIdType.MESH,
        )

    sizes = [0, 0]

    def launch(kind, source, target, recv_sem, peer):
        remote(source, target, sent.at[kind], recv_sem, peer).start()
        sizes[kind] += source.shape[0] * source.shape[1]

    def await_rows(buffer, count, cut, recv_sem):
        where = buffer.at[pl.ds(0, count * rows), cut[0] : cut[1]]
        remote(where, where, recv_sem, recv_sem, core_peer).wait_recv()

    def await_sent(kind):
        rows_sent = sizes[kind] // padded
        assert rows_sent * padded == sizes[kind]
        where = gathered.at[pl.ds(0, rows_sent), :]
        remote(where, where, sent.at[kind], sent.at[kind], core_peer).wait_send()

    def give(origin, chunk, core, q, piece, recv_sem, peer):
        cut = cuts[piece]
        launch(
            0, gathered.at[origin, cut[0] : cut[1]],
            gathered.at[slot(chunk, core, q), cut[0] : cut[1]], recv_sem.at[piece], peer,
        )

    def to_core(chunk, q, piece):
        give(slot(chunk, 0, q), chunk, 1, q, piece, core_sem, core_peer)

    def spread(chunk, piece):
        mode = GATHER[chunk][piece]
        for q in DIRECT[mode]:
            if chunk == 0 and q < 3:
                recv_sem = near_sem
            elif chunk == 1 and q == VIA.get(mode):
                recv_sem = mid_sem
            else:
                recv_sem = late_sem
            give(slot(chunk, 0, 0), chunk, 0, q, piece, recv_sem, quad_peers[q])
        to_core(chunk, 0, piece)

    def relay(chunk, piece):
        mode = GATHER[chunk][piece]
        if mode != "D":
            q = VIA[mode]
            give(slot(chunk, 0, q), chunk, 0, 3, piece, late_sem, quad_peers[3 - q])

    for piece in pieces:
        give(mine, 1, 0, 0, piece, far_sem, far_peer)
        spread(0, piece)

    def take_near(piece):
        await_rows(gathered, 2, cuts[piece], near_sem.at[piece])
        relay(0, piece)
        for q in (2, 1):
            to_core(0, q, piece)

    def take_far(piece):
        await_rows(gathered, 1, cuts[piece], far_sem.at[piece])
        spread(1, piece)

    def take_mid(piece):
        mode = GATHER[1][piece]
        if mode != "D":
            await_rows(gathered, 1, cuts[piece], mid_sem.at[piece])
            relay(1, piece)
            to_core(1, VIA[mode], piece)

    def take_late(piece):
        mode = GATHER[1][piece]
        rest = [q for q in (1, 2, 3) if q != VIA.get(mode)]
        await_rows(gathered, 1 + len(rest), cuts[piece], late_sem.at[piece])
        to_core(0, 3, piece)
        for q in rest:
            to_core(1, q, piece)

    def add_products(piece):
        low_col, high_col = cuts[piece][0], min(cuts[piece][1], width)
        x = gathered[:, low_col:high_col]
        for weight, total in ((vm_gate, gate_sum), (vm_up, up_sum)):
            product = lax.dot_general(
                weight[:, low_col:high_col], x, NT, preferred_element_type=jnp.float32
            )
            total[...] = product if piece == 0 else total[...] + product

    def finish_hidden(piece):
        low_col, high_col = cuts[piece][0], min(cuts[piece][1], width)
        x = gathered[:, low_col:high_col]
        parts = []
        for low_row, high_row in column_cuts(0, vm_gate.shape[0], ROWS):
            g, u = (
                total[low_row:high_row, :] + lax.dot_general(
                    weight[low_row:high_row, low_col:high_col], x, NT,
                    preferred_element_type=jnp.float32,
                )
                for weight, total in ((vm_gate, gate_sum), (vm_up, up_sum))
            )
            parts.append((jax.nn.silu(g) * u).astype(jnp.bfloat16))
        return jnp.concatenate(parts, axis=0)

    def gate_factor():
        info = gathered[:, edge:].astype(jnp.float32)
        factor = jnp.zeros((2 * chunk_rows, 1), jnp.float32)
        for k in range(top):
            col = width - edge + k
            value = info[:, col + top : col + top + 1] + info[:, col + 2 * top : col + 2 * top + 1]
            factor += jnp.where(info[:, col : col + 1] == expert, value, 0.0)
        return factor

    def run_down(hidden, factor, chunk, piece):
        low_out, high_out = out_cuts[piece]
        low_row = chunk * chunk_rows
        high_row = low_row + chunk_rows
        for low_col, high_col in column_cuts(low_out, min(high_out, width), BLOCK):
            y = lax.dot_general(
                hidden[:, low_row:high_row], vm_down[:, low_col:high_col], TN,
                preferred_element_type=jnp.float32,
            )
            part = (y * factor[low_row:high_row]).astype(jnp.bfloat16)
            partial[low_row:high_row, low_col:high_col] = part
        launch(
            1, partial.at[pl.ds(low_row + block_rows, block_rows), low_out:high_out],
            from_core.at[pl.ds(chunk * block_rows, block_rows), low_out:high_out],
            pass_sem.at[chunk, piece], core_peer,
        )

    def chip_sum(chunk, q, piece):
        low_col, high_col = out_cuts[piece]
        mine_part = partial[slot(chunk, 0, q), low_col:high_col].astype(jnp.float32)
        where = pl.ds(chunk * block_rows + q * rows, rows)
        return mine_part + from_core[where, low_col:high_col].astype(jnp.float32)

    def give_sum(total, chunk, q, piece, recv_sem, peer):
        low_col, high_col = out_cuts[piece]
        where = pl.ds((chunk * 3 + q - 1) * rows, rows)
        to_quad[where, low_col:high_col] = total.astype(jnp.bfloat16)
        launch(
            1, to_quad.at[where, low_col:high_col], from_quad.at[where, low_col:high_col],
            recv_sem.at[piece], peer,
        )

    def got(chunk, q, piece):
        low_col, high_col = out_cuts[piece]
        return from_quad[pl.ds((chunk * 3 + q - 1) * rows, rows), low_col:high_col].astype(jnp.float32)

    done_sem = (own_sem, quad_sem)

    def give_out(chunk, q, piece):
        mode = SCATTER[chunk][piece]
        total = chip_sum(chunk, q, piece)
        if q == 3 and mode != "D":
            give_sum(total, chunk, 3, piece, hop_sem.at[chunk], quad_peers[VIA[mode]])
        elif mode == "D" or q == VIA[mode]:
            give_sum(total, chunk, q, piece, done_sem[chunk], quad_peers[q])

    def give_b(piece):
        await_rows(gathered, 4, out_cuts[piece], pass_sem.at[1, piece])
        for q in (3, 1, 2):
            give_out(1, q, piece)

    def relay_out(chunk, piece):
        mode = SCATTER[chunk][piece]
        if mode != "D":
            q = 3 - VIA[mode]
            await_rows(gathered, 1, out_cuts[piece], hop_sem.at[chunk, piece])
            total = chip_sum(chunk, q, piece) + got(chunk, 3, piece)
            give_sum(total, chunk, q, piece, done_sem[chunk], quad_peers[q])

    def quad_total(chunk, piece):
        direct = SCATTER[chunk][piece] == "D"
        await_rows(gathered, 3 if direct else 2, out_cuts[piece], done_sem[chunk].at[piece])
        total = chip_sum(chunk, 0, piece) + got(chunk, 1, piece) + got(chunk, 2, piece)
        return total + got(chunk, 3, piece) if direct else total

    for piece in pieces:
        with jax.named_scope(f"near{piece}"):
            take_near(piece)
        with jax.named_scope(f"far{piece}"):
            take_far(piece)
    for piece in pieces:
        with jax.named_scope(f"mid{piece}"):
            take_mid(piece)
    last = len(cuts) - 1
    def dots(piece):
        with jax.named_scope(f"core{piece}"):
            await_rows(gathered, 8, cuts[piece], core_sem.at[piece])
        with jax.named_scope(f"dot{piece}"):
            add_products(piece)

    for kind, piece in STEPS:
        if kind == "late":
            with jax.named_scope(f"late{piece}"):
                take_late(piece)
            continue
        if piece == 0:
            weights[0].wait()
            weights[1].wait()
        if piece == FACTOR:
            with jax.named_scope("factor"):
                factor = gate_factor()
        if piece < last:
            dots(piece)
    with jax.named_scope(f"core{last}"):
        await_rows(gathered, 8, cuts[last], core_sem.at[last])
    with jax.named_scope("hidden"):
        hidden = finish_hidden(last)
    weights[2].wait()
    with jax.named_scope("down1"):
        for piece in out_pieces:
            run_down(hidden, factor, 1, piece)
    gave = 0
    for piece in out_pieces:
        with jax.named_scope(f"down0_{piece}"):
            run_down(hidden, factor, 0, piece)
        if piece >= GIVE_AT:
            with jax.named_scope(f"give1_{gave}"):
                give_b(gave)
            gave += 1
    for piece in list(out_pieces)[gave:]:
        with jax.named_scope(f"give1_{piece}"):
            give_b(piece)
    for piece in out_pieces:
        await_rows(gathered, 4, out_cuts[piece], pass_sem.at[0, piece])
    with jax.named_scope("give0"):
        for q in (3, 1):
            for piece in out_pieces:
                give_out(0, q, piece)

    def far_out(piece):
        low_col, high_col = out_cuts[piece]
        to_far[:, low_col:high_col] = quad_total(1, piece).astype(jnp.bfloat16)
        launch(
            1, to_far.at[:, low_col:high_col], from_far.at[:, low_col:high_col],
            back_sem.at[piece], far_peer,
        )

    for kind, piece in PLAN:
        with jax.named_scope(f"{kind}{piece}"):
            if kind == "hop":
                relay_out(0, piece)
            elif kind == "pair":
                give_out(0, 2, piece)
            else:
                far_out(piece)
    with jax.named_scope("drain"):
        await_sent(0)
    for piece in out_pieces:
        low_col, high_col = out_cuts[piece]
        with jax.named_scope(f"final{piece}"):
            total = quad_total(0, piece)
        with jax.named_scope(f"end{piece}"):
            await_rows(gathered, 1, out_cuts[piece], back_sem.at[piece])
            total += from_far[:, low_col:high_col].astype(jnp.float32)
            high_col = min(high_col, width)
            out[:, low_col:high_col] = total[:, : high_col - low_col].astype(out.dtype)
    with jax.named_scope("drain_end"):
        await_sent(1)


GIVE_AT = 0
PLAN = (("far", 0), ("far", 1), ("hop", 0), ("far", 2), ("hop", 1), ("hop", 2))
TURN = 1
BLOCK = 1024
FACTOR = 2
ROWS = 240
STEPS = [("late", 0), ("late", 1), ("dot", 0), ("late", 2), ("late", 3), ("dot", 1), ("dot", 2), ("dot", 3)]


def quad_local(tokens, routes, gate_fixed, gate_weight, up_weight, down_weight):
    rows, width = tokens.shape
    top = routes.shape[1]
    gate_weight = jnp.swapaxes(gate_weight, 1, 2)
    up_weight = jnp.swapaxes(up_weight, 1, 2)
    padded = -(-(width + 3 * top) // 128) * 128
    every = 16 * rows
    dma = pltpu.SemaphoreType.DMA
    ins, outs = dma((len(IN_SHARES),)), dma((len(OUT_SHARES),))
    anywhere = pl.BlockSpec(memory_space=pl.ANY)
    routes, gate_fixed = routes.T, gate_fixed.T
    return pl.pallas_call(
        quad_kernel,
        out_shape=pltpu.VMEM((rows, width), jnp.bfloat16),
        in_specs=[anywhere] * 6,
        out_specs=pl.BlockSpec(memory_space=pltpu.VMEM),
        scratch_shapes=[
            pltpu.VMEM(tokens.shape, jnp.bfloat16),
            pltpu.VMEM(routes.shape, jnp.int32),
            pltpu.VMEM(gate_fixed.shape, jnp.int32),
            pltpu.VMEM((every, padded), jnp.bfloat16),
            pltpu.VMEM(gate_weight.shape[1:], jnp.bfloat16),
            pltpu.VMEM(up_weight.shape[1:], jnp.bfloat16),
            pltpu.VMEM(down_weight.shape[1:], jnp.bfloat16),
            pltpu.VMEM((gate_weight.shape[1], every), jnp.float32),
            pltpu.VMEM((gate_weight.shape[1], every), jnp.float32),
            pltpu.VMEM((every, padded), jnp.bfloat16),
            pltpu.VMEM((8 * rows, padded), jnp.bfloat16),
            pltpu.VMEM((6 * rows, padded), jnp.bfloat16),
            pltpu.VMEM((6 * rows, padded), jnp.bfloat16),
            pltpu.VMEM((rows, padded), jnp.bfloat16),
            pltpu.VMEM((rows, padded), jnp.bfloat16),
            dma((3,)), dma((3,)), dma((2,)),
            ins, ins, dma((1,)), ins, ins,
            dma((2, len(OUT_SHARES))), dma((1, len(OUT_SHARES))), outs, outs, outs,
        ],
        compiler_params=pltpu.CompilerParams(
            collective_id=0, has_side_effects=True, vmem_limit_bytes=60 * 2**20
        ),
    )(tokens, routes, gate_fixed, gate_weight, up_weight, down_weight)


def solution(mesh):
    placed = (
        P(("groups", "ep"), None),
        P(("groups", "ep"), None),
        P(("groups", "ep"), None),
        P("ep", None, None),
        P("ep", None, None),
        P("ep", None, None),
    )
    chips = mesh.shape["ep"] // 2

    def body(*args):
        if chips == 2**3:
            return quad_local(*args)
        return local(*args)

    return jax.shard_map(
        body, mesh=mesh, in_specs=placed, out_specs=P(("groups", "ep"), None), check_vma=False
    )
```
